512 devices in a mesh: ens: 4 (over z_lo), replica: 32 (over y_lo, x, core), model: 4 (over z_hi, y_hi).
Axes of the slice: x: 4, y: 8 (y_hi: 2, y_lo: 4; y = y_hi * 4 + y_lo), z: 8 (z_hi: 2, z_lo: 4; z = z_hi * 4 + z_lo), core: 2. Of those that a mesh axis runs over, the one named last changes fastest.
Arguments:
- slope_up: float32 [128, 768, 3072], P(('ens', 'replica'), None, 'model'), parts along dimension 0, may hold values from -1.25 to 1.25
- slope_down: float32 [128, 3072, 768], P(('ens', 'replica'), 'model'), parts along dimension 0, may hold values from -1.25 to 1.25
- slope_norm: float32 [128, 768], P(('ens', 'replica')), parts along dimension 0, may hold values from -12 to 12
- slope_bias: float32 [128, 768], P(('ens', 'replica')), parts along dimension 0, may hold values from -12 to 12
- param_up: float32 [3072, 3072], P(('ens', 'replica'), 'model'), parts along dimension 0, may hold values from -0.4375 to 0.4375
- param_down: float32 [12288, 768], P(('ens', 'model'), 'replica'), parts along dimension 0, may hold values from -0.21875 to 0.21875
- param_norm: float32 [3072], P(('ens', 'replica')), parts along dimension 0, may hold values from 0.25 to 1.75
- param_bias: float32 [3072], P(('ens', 'replica')), parts along dimension 0, may hold values from -3 to 3
Outputs:
- half_up: bfloat16 [3072, 3072], P('ens', 'model'), parts along dimension 0
- half_down: bfloat16 [12288, 768], P(('ens', 'model')), parts along dimension 0
- half_norm: bfloat16 [3072], P('ens'), parts along dimension 0
- half_bias: bfloat16 [3072], P('ens'), parts along dimension 0
- next_up: float32 [3072, 3072], P(('ens', 'replica'), 'model'), parts along dimension 0
- next_down: float32 [12288, 768], P(('ens', 'model'), 'replica'), parts along dimension 0
- next_norm: float32 [3072], P(('ens', 'replica')), parts along dimension 0
- next_bias: float32 [3072], P(('ens', 'replica')), parts along dimension 0
The draws below stay inside these ranges and needn't reach their ends.
There are 4 independent parts, one for each index of `ens`. The reference program is written for one: setup_inputs(seed, part) draws one part's arguments, and reference() takes and returns one part's arrays. A program takes and returns all parts, laid end to end along the dimension named above; each array names one. Nothing has to cross between parts.
All inputs are finite; a program needn't handle non-finite values.
Results may differ from the reference program's by a relative error of at most 0.0004.
Values may be sent and summed in bfloat16 or wider, within the bound.
No kernel may reach another device: no remote copies, remote signals or barrier semaphores. Data moves between devices by JAX's collectives and lax.ppermute only.
A program may use at most 64 MiB of HBM per device.

```python
import jax
import jax.numpy as jnp
from jax import lax

WIDTH = 768
INNER = 3072
REPLICAS = 32


def with_spikes(values, own_key, source, target, parts, factor):
    def block_of(dim):
        return (jnp.arange(values.shape[dim]) // (values.shape[dim] // parts)).reshape((-1,) + (1,) * (values.ndim - 1 - dim))

    one_side = jax.random.permutation(own_key, parts)[block_of(target)]
    second = (block_of(target) + parts // 2) % parts
    return jnp.where((block_of(source) == one_side) | (block_of(source) == second), factor * values, values)


def block_scale(key, extent, split, smallest, largest):
    factor_of, own = 1.0, jax.random.fold_in(key, 6)
    for axis_at, parts in split:
        heights = jnp.exp(jax.random.uniform(jax.random.fold_in(own, axis_at), (parts,), jnp.float32, smallest / len(split), largest / len(split)))
        factor_of = factor_of * jnp.repeat(heights, extent[axis_at] // parts).reshape([-1 if axis == axis_at else 1 for axis in range(len(extent))])
    return factor_of


def gaussian(key, shape, width, most, cuts=(), dtype=jnp.bfloat16):
    factor_of = block_scale(key, shape, cuts, -0.22, 0.18) if cuts else 1.0
    result = jax.random.normal(key, shape, jnp.float32) * width * factor_of
    return jnp.minimum(jnp.maximum(result, -most), most).astype(dtype)


def bell_draw_with(own_key, extent, deviation, reach, cuts, heavy, dtype=jnp.bfloat16):
    result = deviation * jax.random.normal(own_key, extent, jnp.float32)
    if cuts:
        result = result * block_scale(own_key, extent, cuts, -0.22, 0.18)
    return jnp.clip(with_spikes(result, jax.random.fold_in(own_key, 3), *heavy), -reach, reach).astype(dtype)


def setup_inputs(seed: int = 0, part: int = 0) -> dict:
    splits = jax.random.split(jax.random.key(seed), 9)
    own_keys = jax.random.split(jax.random.fold_in(splits[8], part), 9)
    return {
        "slope_up": bell_draw_with(own_keys[0], (REPLICAS, WIDTH, INNER), 0.1, 1.25, ((0, 32), (2, 4)), (0, 1, 32, 2.75), jnp.float32),
        "slope_down": bell_draw_with(own_keys[1], (REPLICAS, INNER, WIDTH), 0.1, 1.25, ((0, 32), (1, 4)), (0, 2, 32, 2.75), jnp.float32),
        "slope_norm": bell_draw_with(own_keys[2], (REPLICAS, WIDTH), 1.0, 12.0, ((0, 32),), (0, 1, 32, 2.75), jnp.float32),
        "slope_bias": bell_draw_with(own_keys[3], (REPLICAS, WIDTH), 1.0, 12.0, ((0, 32),), (0, 1, 32, 2.75), jnp.float32),
        "param_up": bell_draw_with(own_keys[4], (WIDTH, INNER), WIDTH ** -0.5, 0.4375, ((0, 32), (1, 4)), (1, 0, 32, 2.75), jnp.float32),
        "param_down": bell_draw_with(own_keys[5], (INNER, WIDTH), INNER ** -0.5, 0.21875, ((0, 4), (1, 32)), (0, 1, 32, 2.75), jnp.float32),
        "param_norm": jnp.clip(1.0 + 0.15 * jax.random.normal(own_keys[6], (WIDTH,), jnp.float32), 0.25, 1.75),
        "param_bias": gaussian(own_keys[7], (WIDTH,), 0.5, 3.0, ((0, 32),), jnp.float32),
    }


learn_rate = 0.4

def reference(slope_up, slope_down, slope_norm, slope_bias, param_up, param_down, param_norm, param_bias):
    mean_up = lax.optimization_barrier(jnp.sum(slope_up.astype(jnp.float32), axis=0)) * REPLICAS ** (-0.5)
    mean_down = lax.optimization_barrier(jnp.sum(slope_down.astype(jnp.float32), axis=0)) * REPLICAS ** (-0.5)
    mean_norm = lax.optimization_barrier(jnp.sum(slope_norm.astype(jnp.float32), axis=0)) * REPLICAS ** (-0.5)
    mean_bias = lax.optimization_barrier(jnp.sum(slope_bias.astype(jnp.float32), axis=0)) * REPLICAS ** (-0.5)
    ratio_up = jnp.sqrt(lax.optimization_barrier(jnp.sum(param_up * param_up, axis=1, keepdims=True))) * lax.rsqrt(lax.optimization_barrier(jnp.sum(mean_up * mean_up, axis=1, keepdims=True)) + 1e-06)
    mean_up = mean_up * ratio_up
    ratio_down = jnp.sqrt(lax.optimization_barrier(jnp.sum(param_down * param_down, axis=0, keepdims=True))) * lax.rsqrt(lax.optimization_barrier(jnp.sum(mean_down * mean_down, axis=0, keepdims=True)) + 1e-06)
    mean_down = mean_down * ratio_down
    next_up = param_up - learn_rate * mean_up
    next_down = param_down - learn_rate * mean_down
    next_norm = param_norm - learn_rate * mean_norm
    next_bias = param_bias - learn_rate * mean_bias
    half_up = next_up.astype(jnp.bfloat16)
    half_down = next_down.astype(jnp.bfloat16)
    half_norm = next_norm.astype(jnp.bfloat16)
    half_bias = next_bias.astype(jnp.bfloat16)
    return (half_up, half_down, half_norm, half_bias, next_up, next_down, next_norm, next_bias)
```

```python
import jax
import jax.numpy as jnp
from jax import lax
from jax.sharding import Mesh
from jax.sharding import PartitionSpec as P

REPLICA = ("y", "x", "core")
ENS_REPLICA = ("ens", "y", "x", "core")
PLANE = ("y", "x")
MODEL = ("mz", "my")
SWAP = [(0, 1), (1, 0)]

learn_rate = 0.4
f32 = jnp.float32
SPAN = 173.25


def core_sum(grad):
    core = lax.axis_index("core")
    tiles = grad.reshape(16, 2, 24, 768)
    mine = lax.dynamic_index_in_dim(tiles, core, 1, keepdims=False)
    other = lax.dynamic_index_in_dim(tiles, 1 - core, 1, keepdims=False)
    return mine + lax.ppermute(other, "core", SWAP)


def encode(part):
    top = jnp.max(jnp.abs(part), axis=2, keepdims=True)
    top = lax.reduce_precision(jnp.maximum(top, 1e-30) * (1 + 2.0**-7), 8, 7)
    code = jnp.exp(jnp.abs(part) * (SPAN / top) - SPAN / 2)
    code = jnp.where(part < 0, -code, code)
    return jnp.concatenate([code, jnp.broadcast_to(top, (16, 24, 128))], axis=2).astype(jnp.bfloat16)


def decode(message):
    code = message[:, :, :768].astype(f32)
    top = message[:, :, 768:769].astype(f32)
    size = (jnp.log(jnp.abs(code)) + SPAN / 2) * (top * (1 / SPAN))
    return jnp.where(code < 0, -size, size)


def plane_sum(part):
    return jnp.sum(decode(lax.all_to_all(encode(part), PLANE, 0, 0, tiled=True)), axis=0) * 32**-0.5


def model_sum(a):
    a = a + lax.ppermute(a, "mz", SWAP)
    return a + lax.ppermute(a, "my", SWAP)


def step(param, mean):
    sizes = jnp.stack([jnp.sum(param * param, axis=1), jnp.sum(mean * mean, axis=1)])
    sizes = model_sum(sizes)
    ratio = jnp.sqrt(sizes[0]) * lax.rsqrt(sizes[1] + 1e-06)
    return param - learn_rate * (mean * ratio[:, None])


def gather(rows):
    core = lax.axis_index("core")
    plane = lax.all_to_all(jnp.broadcast_to(rows[None], (16, 24, 768)), PLANE, 0, 0, tiled=True)
    got = lax.ppermute(plane, "core", SWAP)
    return jnp.stack([jnp.where(core == 0, plane, got), jnp.where(core == 0, got, plane)], axis=1)


def small_sums(slope_norm, slope_bias, param_norm, param_bias):
    own = jnp.concatenate([slope_norm.reshape(6, 128), slope_bias.reshape(6, 128),
                           jnp.concatenate([param_norm, param_bias, jnp.zeros(80, f32)]).reshape(1, 128)])
    every = lax.all_to_all(jnp.broadcast_to(own[None], (32, 13, 128)), REPLICA, 0, 0, tiled=True)
    sums = jnp.sum(every[:, :12], axis=0) * 32**-0.5
    params = every[:, 12]
    norm = params[:, :24].reshape(768) - learn_rate * sums[:6].reshape(768)
    bias = params[:, 24:48].reshape(768) - learn_rate * sums[6:].reshape(768)
    return norm, bias


def on_device(
    slope_up, slope_down, slope_norm, slope_bias, param_up, param_down, param_norm, param_bias
):
    norm, bias = small_sums(slope_norm[0], slope_bias[0], param_norm, param_bias)
    up = core_sum(slope_up[0])
    down = core_sum(slope_down[0].T)
    mean_up = plane_sum(up)
    mean_down = plane_sum(down)
    next_up = step(param_up, mean_up)
    half_up = gather(next_up.astype(jnp.bfloat16)).reshape(768, 768)
    turned = step(param_down.T, mean_down)
    half_down = gather(turned.astype(jnp.bfloat16)).reshape(768, 768).T
    r = lax.axis_index(REPLICA)
    next_norm = lax.dynamic_slice_in_dim(norm, 24 * r, 24)
    next_bias = lax.dynamic_slice_in_dim(bias, 24 * r, 24)
    bf = jnp.bfloat16
    return half_up, half_down, norm.astype(bf), bias.astype(bf), next_up, turned.T, next_norm, next_bias


def solution(mesh):
    split = Mesh(
        mesh.devices.reshape(mesh.shape["ens"], 4, 4, 2, 2, 2),
        ("ens", "y", "x", "core", "mz", "my"),
    )
    return jax.shard_map(
        on_device,
        mesh=split,
        in_specs=(
            P(ENS_REPLICA, None, MODEL),
            P(ENS_REPLICA, MODEL, None),
            P(ENS_REPLICA, None),
            P(ENS_REPLICA, None),
            P(ENS_REPLICA, MODEL),
            P(("ens", *MODEL), REPLICA),
            P(ENS_REPLICA),
            P(ENS_REPLICA),
        ),
        out_specs=(
            P("ens", MODEL),
            P(("ens", *MODEL), None),
            P("ens"),
            P("ens"),
            P(ENS_REPLICA, MODEL),
            P(("ens", *MODEL), REPLICA),
            P(ENS_REPLICA),
            P(ENS_REPLICA),
        ),
        check_vma=False,
    )
```

```python
import jax
import jax.numpy as jnp
from jax import lax
from jax.experimental import pallas as pl
from jax.experimental.pallas import tpu as pltpu
from jax.sharding import Mesh
from jax.sharding import PartitionSpec as P


ENS_REPLICA = ("ens", "y", "x", "core")
PLANE = ("y", "x")
MODEL = ("mz", "my")
SWAP = [(0, 1), (1, 0)]

learn_rate = 0.4
f32 = jnp.float32
bf16 = jnp.bfloat16
SPAN = 173.25
GROUP = 4
VMEM = pl.BlockSpec(memory_space=pltpu.VMEM)
PARAMS = pltpu.CompilerParams(vmem_limit_bytes=12 << 20)


def pieces(a):
    high = a.astype(bf16).astype(f32)
    rest = a - high
    middle = rest.astype(bf16).astype(f32)
    return high, middle, rest - middle


def pick_kernel(core_ref, tiles_ref, vector_ref, param_ref, out_ref):
    i = pl.program_id(0)

    @pl.when(i < 4)
    def _():
        out_ref[...] = tiles_ref[0, :, 0]

    @pl.when(i == 4)
    def _():
        out_ref[0, 0:8, :] = jnp.broadcast_to(vector_ref[...], (8, 768))
        out_ref[0, 8:16, 0:128] = jnp.broadcast_to(param_ref[...], (8, 128))


def pick(core, grad, vector, param):
    return pl.pallas_call(
        pick_kernel,
        grid_spec=pltpu.PrefetchScalarGridSpec(
            num_scalar_prefetch=1,
            grid=(5,),
            in_specs=[
                pl.BlockSpec((1, GROUP, 1, 24, 768), lambda i, c: (jnp.minimum(i, 3), 0, 1 - c[0], 0, 0)),
                pl.BlockSpec((1, 768), lambda i, c: (0, 0)),
                pl.BlockSpec((1, 128), lambda i, c: (0, 0)),
            ],
            out_specs=pl.BlockSpec((GROUP, 24, 768), lambda i, c: (i, 0, 0)),
        ),
        out_shape=jax.ShapeDtypeStruct((17, 24, 768), f32),
        compiler_params=PARAMS,
        name="pick",
    )(core, grad.reshape(4, GROUP, 2, 24, 768), vector, param)


def encode_kernel(core_ref, tiles_ref, got_ref, small_ref, vector_ref, param_ref, out_ref):
    core = core_ref[0]
    total = vector_ref[...] + small_ref[0, 0:1, :]
    wide = [jnp.concatenate([total[:, 96 * k : 96 * k + 96], jnp.zeros((1, 32), f32)], axis=1) for k in range(8)]
    mine = jnp.broadcast_to(param_ref[...], (8, 128))
    theirs = jnp.broadcast_to(small_ref[0, 8:9, 0:128], (8, 128))
    parts = pieces(jnp.concatenate(wide, axis=0))
    first = pieces(jnp.where(core == 0, mine, theirs))
    second = pieces(jnp.where(core == 0, theirs, mine))
    row = lax.broadcasted_iota(jnp.int32, (8, 128), 0)
    listed = jnp.zeros((8, 128), f32)
    for k, a in enumerate((*first, *second)):
        listed = jnp.where(row == k, a, listed)
    lane = lax.broadcasted_iota(jnp.int32, (8, 128), 1)
    beside = jnp.concatenate([jnp.where(lane >= 100, listed, parts[0]), parts[1], parts[2]], axis=0)
    lane = lax.broadcasted_iota(jnp.int32, (24, 128), 1)
    for o in range(GROUP):
        part = tiles_ref[0, o, 0] + got_ref[o]
        size = jnp.abs(part)
        top = jnp.max(size, axis=1, keepdims=True)
        top = (jnp.maximum(top, 1e-30) * (1 + 2.0**-7)).astype(bf16).astype(f32)
        code = jnp.exp(size * (SPAN / top) - SPAN / 2)
        code = jnp.where(part < 0, -code, code)
        out_ref[o, :, 0:768] = code.astype(bf16)
        out_ref[o, :, 768:896] = jnp.where(lane == 96, top, beside).astype(bf16)


def encode(core, grad, got, vector, param):
    return pl.pallas_call(
        encode_kernel,
        grid_spec=pltpu.PrefetchScalarGridSpec(
            num_scalar_prefetch=1,
            grid=(4,),
            in_specs=[
                pl.BlockSpec((1, GROUP, 1, 24, 768), lambda i, c: (i, 0, c[0], 0, 0)),
                pl.BlockSpec((GROUP, 24, 768), lambda i, c: (i, 0, 0)),
                pl.BlockSpec((1, 24, 768), lambda i, c: (16, 0, 0)),
                pl.BlockSpec((1, 768), lambda i, c: (0, 0)),
                pl.BlockSpec((1, 128), lambda i, c: (0, 0)),
            ],
            out_specs=pl.BlockSpec((GROUP, 24, 896), lambda i, c: (i, 0, 0)),
        ),
        out_shape=jax.ShapeDtypeStruct((16, 24, 896), bf16),
        compiler_params=PARAMS,
        name="encode",
    )(core, grad.reshape(4, GROUP, 2, 24, 768), got, got, vector, param)


def decode_kernel(message_ref, param_ref, mean_ref, sizes_ref, vector_ref, params_ref):
    def add(o, carry):
        total, beside = carry
        code = message_ref[o, :, 0:768].astype(f32)
        side = message_ref[o, :, 768:896].astype(f32)
        params_ref[o] = side[0:8, :]
        size = (jnp.log(jnp.abs(code)) + SPAN / 2) * (side[:, 96:97] * (1 / SPAN))
        return total + jnp.where(code < 0, -size, size), beside + side

    start = (jnp.zeros((24, 768), f32), jnp.zeros((24, 128), f32))
    total, beside = lax.fori_loop(0, 16, add, start)
    mean = total * 32**-0.5
    param = param_ref[...]
    mean_ref[...] = mean
    vector_ref[...] = beside[0:8] + beside[8:16] + beside[16:24]
    own = jnp.sum(param * param, axis=1, keepdims=True)
    size = jnp.sum(mean * mean, axis=1, keepdims=True)
    lane = lax.broadcasted_iota(jnp.int32, (24, 128), 1)
    sizes_ref[...] = jnp.where(lane < 64, own, size)


def decode(message, param):
    return pl.pallas_call(
        decode_kernel,
        out_shape=(
            jax.ShapeDtypeStruct((24, 768), f32),
            jax.ShapeDtypeStruct((24, 128), f32),
            jax.ShapeDtypeStruct((8, 128), f32),
            jax.ShapeDtypeStruct((16, 8, 128), f32),
        ),
        in_specs=[VMEM] * 2,
        out_specs=(VMEM,) * 4,
        compiler_params=PARAMS,
        name="decode",
    )(message, param)


def step_kernel(param_ref, mean_ref, near_ref, far_ref, next_ref, copies_ref):
    sizes = near_ref[...] + far_ref[...]
    ratio = jnp.sqrt(sizes[:, 0:1]) * lax.rsqrt(sizes[:, 64:65] + 1e-06)
    after = param_ref[...] - learn_rate * (mean_ref[...] * ratio)
    next_ref[...] = after
    half = after.astype(bf16)
    for o in range(16):
        copies_ref[o] = half


def step(param, mean, near, far):
    return pl.pallas_call(
        step_kernel,
        out_shape=(jax.ShapeDtypeStruct((24, 768), f32), jax.ShapeDtypeStruct((16, 24, 768), bf16)),
        in_specs=[VMEM] * 4,
        out_specs=(VMEM, VMEM),
        compiler_params=PARAMS,
        name="step",
    )(param, mean, near, far)


def merge_kernel(core_ref, plane_ref, got_ref, out_ref):
    core = core_ref[0]
    out_ref[0, :, pl.ds(core, 1)] = plane_ref[...][:, None]
    out_ref[0, :, pl.ds(1 - core, 1)] = got_ref[...][:, None]


def merge(core, plane, got):
    whole = pl.pallas_call(
        merge_kernel,
        grid_spec=pltpu.PrefetchScalarGridSpec(
            num_scalar_prefetch=1,
            grid=(4,),
            in_specs=[pl.BlockSpec((GROUP, 24, 768), lambda i, c: (i, 0, 0))] * 2,
            out_specs=pl.BlockSpec((1, GROUP, 2, 24, 768), lambda i, c: (i, 0, 0, 0, 0)),
        ),
        out_shape=jax.ShapeDtypeStruct((4, GROUP, 2, 24, 768), bf16),
        compiler_params=PARAMS,
        name="merge",
    )(core, plane, got)
    return whole.reshape(768, 768)


def vector_step(beside, params):
    total = beside[:, 0:96].reshape(768)
    first = params[:, 0:1, 100:124] + params[:, 1:2, 100:124] + params[:, 2:3, 100:124]
    second = params[:, 3:4, 100:124] + params[:, 4:5, 100:124] + params[:, 5:6, 100:124]
    param = jnp.concatenate([first, second], axis=1).reshape(768)
    return param - learn_rate * (total * 32**-0.5)


def on_device(
    slope_up, slope_down, slope_norm, slope_bias, param_up, param_down, param_norm, param_bias
):
    core = lax.axis_index("core").astype(jnp.int32)
    cores = core.reshape(1)
    padded = jnp.pad(jnp.stack([param_norm, param_bias]), ((0, 0), (100, 4)))
    streams = {
        "up": (slope_up[0], param_up, slope_norm, padded[0:1]),
        "down": (slope_down[0].T, param_down.T, slope_bias, padded[1:2]),
    }
    messages, vectors, copies, after, halves = {}, {}, {}, {}, {}
    for s, (grad, _, vector, small) in streams.items():
        got = lax.ppermute(pick(cores, grad, vector, small), "core", SWAP)
        messages[s] = encode(cores, grad, got, vector, small)
    for s, (_, param, _, _) in streams.items():
        arrived = lax.all_to_all(messages[s], PLANE, 0, 0, tiled=True)
        mean, sizes, beside, params = decode(arrived, param)
        near = sizes + lax.ppermute(sizes, "mz", SWAP)
        far = lax.ppermute(near, "my", SWAP)
        after[s], copies[s] = step(param, mean, near, far)
        vectors[s] = vector_step(beside, params)
    for s in streams:
        plane = lax.all_to_all(copies[s], PLANE, 0, 0, tiled=True)
        got = lax.ppermute(plane, "core", SWAP)
        halves[s] = merge(cores, plane, got)
    at = 24 * lax.axis_index(("y", "x", "core"))
    own_norm = lax.dynamic_slice_in_dim(vectors["up"], at, 24)
    own_bias = lax.dynamic_slice_in_dim(vectors["down"], at, 24)
    return (
        halves["up"], halves["down"].T, vectors["up"].astype(bf16), vectors["down"].astype(bf16),
        after["up"], after["down"].T, own_norm, own_bias,
    )


def solution(mesh):
    split = Mesh(
        mesh.devices.reshape(mesh.shape["ens"], 4, 4, 2, 2, 2),
        ("ens", "y", "x", "core", "mz", "my"),
    )

    return jax.shard_map(
        on_device,
        mesh=split,
        in_specs=(
            P(ENS_REPLICA, None, MODEL),
            P(ENS_REPLICA, MODEL, None),
            P(ENS_REPLICA, None),
            P(ENS_REPLICA, None),
            P(ENS_REPLICA, MODEL),
            P(("ens", *MODEL), ("y", "x", "core")),
            P(ENS_REPLICA),
            P(ENS_REPLICA),
        ),
        out_specs=(
            P("ens", MODEL),
            P(("ens", *MODEL), None),
            P("ens"),
            P("ens"),
            P(ENS_REPLICA, MODEL),
            P(("ens", *MODEL), ("y", "x", "core")),
            P(ENS_REPLICA),
            P(ENS_REPLICA),
        ),
        check_vma=False,
    )
```

```python
import jax
import jax.numpy as jnp
from jax import lax
from jax.experimental import pallas as pl
from jax.experimental.pallas import tpu as pltpu
from jax.sharding import Mesh
from jax.sharding import PartitionSpec as P

ENS_REPLICA = ("ens", "y", "x", "core")
MODEL = ("mz", "my")
SWAP = [(0, 1), (1, 0)]

learn_rate = 0.4
f32 = jnp.float32
bf16 = jnp.bfloat16
SPAN = 173.25
VMEM = pl.BlockSpec(memory_space=pltpu.VMEM)
PARAMS = pltpu.CompilerParams(vmem_limit_bytes=12 << 20)


def shape(*dims, dtype=f32):
    return jax.ShapeDtypeStruct(dims, dtype)


def call(kernel, out_shape, count):
    return pl.pallas_call(
        kernel,
        in_specs=[VMEM] * count,
        out_specs=jax.tree.map(lambda _: VMEM, out_shape),
        out_shape=out_shape,
        compiler_params=PARAMS,
    )


def pieces(a):
    high = a.astype(bf16).astype(f32)
    rest = a - high
    middle = rest.astype(bf16).astype(f32)
    return high, middle, rest - middle


def encode_rows(part, beside):
    size = jnp.abs(part)
    top = jnp.max(size, axis=1, keepdims=True)
    top = (jnp.maximum(top, 1e-30) * (1 + 2.0**-7)).astype(bf16).astype(f32)
    code = jnp.exp(size * (SPAN / top) - SPAN / 2)
    code = jnp.where(part < 0, -code, code)
    lane = lax.broadcasted_iota(jnp.int32, (24, 128), 1)
    return code.astype(bf16), jnp.where(lane == 96, top, beside).astype(bf16)


def decode_rows(code, side):
    code = code.astype(f32)
    size = (jnp.log(jnp.abs(code)) + SPAN / 2) * (side[:, 96:97] * (1 / SPAN))
    return jnp.where(code < 0, -size, size)


def placed(param):
    wide = jnp.concatenate([jnp.zeros((1, 100), f32), param, jnp.zeros((1, 4), f32)], axis=1)
    return jnp.broadcast_to(wide, (8, 128))


def pick_kernel(core_ref, tiles_ref, vector_ref, param_ref, out_ref):
    i = pl.program_id(0)

    @pl.when(i < 4)
    def _():
        out_ref[...] = tiles_ref[0, :, 0]

    @pl.when(i == 4)
    def _():
        out_ref[0, 0:8, :] = jnp.broadcast_to(vector_ref[...], (8, 768))
        out_ref[0, 8:16, 0:128] = placed(param_ref[...])


def pick(core, grad, vector, param):
    return pl.pallas_call(
        pick_kernel,
        grid_spec=pltpu.PrefetchScalarGridSpec(
            num_scalar_prefetch=1,
            grid=(5,),
            in_specs=[
                pl.BlockSpec((1, 4, 1, 24, 768), lambda i, c: (jnp.minimum(i, 3), 0, 1 - c[0], 0, 0)),
                pl.BlockSpec((1, 768), lambda i, c: (0, 0)),
                pl.BlockSpec((1, 24), lambda i, c: (0, 0)),
            ],
            out_specs=pl.BlockSpec((4, 24, 768), lambda i, c: (i, 0, 0)),
        ),
        out_shape=shape(17, 24, 768),
        compiler_params=PARAMS,
        name="pick",
    )(core, grad.reshape(4, 4, 2, 24, 768), vector, param)


def encode_kernel(core_ref, tiles_ref, got_ref, small_ref, vector_ref, param_ref, *refs):
    out_ref = refs[-1]
    core = core_ref[0]
    total = vector_ref[...] + small_ref[0, 0:1, :]
    wide = [jnp.concatenate([total[:, 96 * k : 96 * k + 96], jnp.zeros((1, 32), f32)], axis=1) for k in range(8)]
    mine = placed(param_ref[...])
    theirs = jnp.broadcast_to(small_ref[0, 8:9, 0:128], (8, 128))
    parts = pieces(jnp.concatenate(wide, axis=0))
    first = pieces(jnp.where(core == 0, mine, theirs))
    second = pieces(jnp.where(core == 0, theirs, mine))
    row = lax.broadcasted_iota(jnp.int32, (8, 128), 0)
    listed = jnp.zeros((8, 128), f32)
    for k, a in enumerate((*first, *second)):
        listed = jnp.where(row == k, a, listed)
    lane = lax.broadcasted_iota(jnp.int32, (8, 128), 1)
    beside = jnp.concatenate([jnp.where(lane >= 100, listed, parts[0]), parts[1], parts[2]], axis=0)
    for x in range(4):
        out_ref[x, :, 0:768], out_ref[x, :, 768:896] = encode_rows(tiles_ref[0, x, 0] + got_ref[x], beside)


def encode(core, grad, got, vector, param, message=None):
    t = int(message is not None)
    return pl.pallas_call(
        encode_kernel,
        grid_spec=pltpu.PrefetchScalarGridSpec(
            num_scalar_prefetch=1,
            grid=(4,),
            in_specs=[
                pl.BlockSpec((1, 4, 1, 24, 768), lambda i, c: (i, 0, c[0], 0, 0)),
                pl.BlockSpec((4, 24, 768), lambda i, c: (i, 0, 0)),
                pl.BlockSpec((1, 24, 768), lambda i, c: (16, 0, 0)),
                pl.BlockSpec((1, 768), lambda i, c: (0, 0)),
                pl.BlockSpec((1, 24), lambda i, c: (0, 0)),
            ] + [pl.BlockSpec(memory_space=pl.ANY)] * t,
            out_specs=pl.BlockSpec((4, 24, 896), lambda i, c: (0, 2 * i + t, 0)),
        ),
        out_shape=shape(4, 192, 896, dtype=bf16),
        input_output_aliases={6: 0} if t else {},
        compiler_params=PARAMS,
        name="encode",
    )(core, grad.reshape(4, 4, 2, 24, 768), got, got, vector, param, *([message] * t))


def recode_kernel(message_ref, out_ref):
    lane = lax.broadcasted_iota(jnp.int32, (24, 128), 1)
    to, at = (lax.broadcasted_iota(jnp.int32, (24, 24), d) for d in (0, 1))
    for t in range(2):
        vector = jnp.zeros((8, 128), f32)
        listed = jnp.zeros((24, 128), f32)
        for x in range(4):
            side = message_ref[x, 24 * t : 24 * t + 24, 768:896]
            wide = side.astype(f32)
            vector = vector + (wide[0:8] + wide[8:16] + wide[16:24])
            chosen = ((to == at + 6 * x) & (at < 6)).astype(bf16)
            listed = listed + jnp.dot(chosen, side, preferred_element_type=f32)
        beside = jnp.where(lane >= 100, listed, jnp.concatenate(pieces(vector), axis=0))
        for y in range(4):
            rows = slice(48 * y + 24 * t, 48 * y + 24 * t + 24)
            part = jnp.zeros((24, 768), f32)
            for x in range(4):
                part = part + decode_rows(message_ref[x, rows, 0:768], message_ref[x, rows, 768:896].astype(f32))
            to_y = slice(24 * t, 24 * t + 24)
            out_ref[y, to_y, 0:768], out_ref[y, to_y, 768:896] = encode_rows(part, beside)


def decode_kernel(message_ref, up_ref, down_ref, mean_ref, sizes_ref, vector_ref, params_ref):
    lane = lax.broadcasted_iota(jnp.int32, (24, 128), 1)
    for t, param_ref in enumerate((up_ref, down_ref)):
        rows = slice(24 * t, 24 * t + 24)
        total = jnp.zeros((24, 768), f32)
        beside = jnp.zeros((24, 128), f32)
        for y in range(4):
            side = message_ref[y, rows, 768:896].astype(f32)
            params_ref[t, y] = side
            beside = beside + side
            total = total + decode_rows(message_ref[y, rows, 0:768], side)
        mean = total * 32**-0.5
        mean_ref[rows] = mean
        vector_ref[t] = beside[0:8] + beside[8:16] + beside[16:24]
        param = param_ref[...]
        own = jnp.sum(param * param, axis=1, keepdims=True)
        size = jnp.sum(mean * mean, axis=1, keepdims=True)
        both = jnp.where(lane < 64, own, size)
        for m in range(4):
            sizes_ref[m, rows] = both


def step_kernel(up_ref, down_ref, mean_ref, sizes_ref, next_up_ref, next_down_ref, copies_ref):
    for t, (param_ref, next_ref) in enumerate(((up_ref, next_up_ref), (down_ref, next_down_ref))):
        rows = slice(24 * t, 24 * t + 24)
        sizes = (sizes_ref[0, rows] + sizes_ref[1, rows]) + (sizes_ref[2, rows] + sizes_ref[3, rows])
        ratio = jnp.sqrt(sizes[:, 0:1]) * lax.rsqrt(sizes[:, 64:65] + 1e-06)
        after = param_ref[...] - learn_rate * (mean_ref[rows] * ratio)
        next_ref[...] = after
        half = after.astype(bf16)
        for y in range(4):
            copies_ref[y, rows] = half


def merge_kernel(core_ref, plane_ref, got_ref, up_ref, down_ref):
    core = core_ref[0]
    for ref, at in ((plane_ref, core), (got_ref, 1 - core)):
        for x in range(4):
            up_ref[0, x, pl.ds(at, 1)] = ref[x, :, 0:24]
            down_ref[0, x, pl.ds(at, 1)] = ref[x, :, 24:48]


def merge(core, plane, got):
    out = pl.BlockSpec((1, 4, 2, 24, 768), lambda i, c: (i, 0, 0, 0, 0))
    up, down = pl.pallas_call(
        merge_kernel,
        grid_spec=pltpu.PrefetchScalarGridSpec(
            num_scalar_prefetch=1,
            grid=(4,),
            in_specs=[pl.BlockSpec((4, 1, 48, 768), lambda i, c: (0, i, 0, 0))] * 2,
            out_specs=(out, out),
        ),
        out_shape=(shape(4, 4, 2, 24, 768, dtype=bf16),) * 2,
        compiler_params=PARAMS,
        name="merge",
    )(core, plane, got)
    return up.reshape(768, 768), down.reshape(768, 768)


def vector_kernel(vectors_ref, params_ref, out_ref):
    for t in range(2):
        total = jnp.concatenate([vectors_ref[t, k : k + 1, 0:96] for k in range(8)], axis=1)
        listed = []
        for y in range(4):
            for k in range(0, 24, 3):
                param = params_ref[t, y, k : k + 1] + params_ref[t, y, k + 1 : k + 2] + params_ref[t, y, k + 2 : k + 3]
                listed.append(param[:, 100:124])
        out_ref[t : t + 1] = jnp.concatenate(listed, axis=1) - learn_rate * (total * 32**-0.5)


def exchange(a, axis):
    return lax.all_to_all(a, axis, 0, 0, tiled=True)


def on_device(
    slope_up, slope_down, slope_norm, slope_bias, param_up, param_down, param_norm, param_bias
):
    cores = lax.axis_index("core").astype(jnp.int32).reshape(1)
    turned = param_down.T
    message = None
    for grad, vector, param in ((slope_up[0], slope_norm, param_norm), (slope_down[0].T, slope_bias, param_bias)):
        param = param.reshape(1, 24)
        got = lax.ppermute(pick(cores, grad, vector, param), "core", SWAP)
        message = encode(cores, grad, got, vector, param, message)
    recoded = call(recode_kernel, shape(4, 48, 896, dtype=bf16), 1)(exchange(message, "x"))
    outs = (shape(48, 768), shape(4, 48, 128), shape(2, 8, 128), shape(2, 4, 24, 128))
    mean, sizes, vectors, params = call(decode_kernel, outs, 3)(exchange(recoded, "y"), param_up, turned)
    outs = (shape(24, 768), shape(24, 768), shape(4, 48, 768, dtype=bf16))
    next_up, next_down, copies = call(step_kernel, outs, 4)(param_up, turned, mean, exchange(sizes, MODEL))
    rows = exchange(copies, "y")
    norm, bias = call(vector_kernel, shape(2, 768), 2)(vectors, params)
    at = 24 * lax.axis_index(("y", "x", "core"))
    small = (
        norm.astype(bf16), bias.astype(bf16),
        lax.dynamic_slice_in_dim(norm, at, 24), lax.dynamic_slice_in_dim(bias, at, 24),
    )
    plane = exchange(jnp.broadcast_to(rows[None], (4, 4, 48, 768)), "x")
    plane, half_norm, half_bias, next_norm, next_bias = lax.optimization_barrier((plane, *small))
    half_up, half_down = merge(cores, plane, lax.ppermute(plane, "core", SWAP))
    return half_up, half_down.T, half_norm, half_bias, next_up, next_down.T, next_norm, next_bias


def solution(mesh):
    split = Mesh(
        mesh.devices.reshape(mesh.shape["ens"], 4, 4, 2, 2, 2),
        ("ens", "y", "x", "core", "mz", "my"),
    )
    return jax.shard_map(
        on_device,
        mesh=split,
        in_specs=(
            P(ENS_REPLICA, None, MODEL),
            P(ENS_REPLICA, MODEL, None),
            P(ENS_REPLICA, None),
            P(ENS_REPLICA, None),
            P(ENS_REPLICA, MODEL),
            P(("ens", *MODEL), ("y", "x", "core")),
            P(ENS_REPLICA),
            P(ENS_REPLICA),
        ),
        out_specs=(
            P("ens", MODEL),
            P(("ens", *MODEL), None),
            P("ens"),
            P("ens"),
            P(ENS_REPLICA, MODEL),
            P(("ens", *MODEL), ("y", "x", "core")),
            P(ENS_REPLICA),
            P(ENS_REPLICA),
        ),
        check_vma=False,
    )
```

```python
import jax
import jax.numpy as jnp
from jax import lax
from jax.experimental import pallas as pl
from jax.experimental.pallas import tpu as pltpu
from jax.sharding import Mesh
from jax.sharding import PartitionSpec as P

ENS_REPLICA = ("ens", "y", "x", "core")
MODEL = ("mz", "my")
SWAP = [(0, 1), (1, 0)]

learn_rate = 0.4
f32 = jnp.float32
bf16 = jnp.bfloat16
SPAN = 173.25
VMEM = pl.BlockSpec(memory_space=pltpu.VMEM)
PARAMS = pltpu.CompilerParams(vmem_limit_bytes=12 << 20)


def in_hbm(*arrays):
    return [pltpu.with_memory_space_constraint(a, pltpu.HBM) for a in arrays]


def shape(*dims, dtype=f32):
    return jax.ShapeDtypeStruct(dims, dtype)


def call(kernel, out_shape, count):
    return pl.pallas_call(
        kernel,
        in_specs=[VMEM] * count,
        out_specs=jax.tree.map(lambda _: VMEM, out_shape),
        out_shape=out_shape,
        compiler_params=PARAMS,
    )


def pieces(a):
    high = a.astype(bf16).astype(f32)
    rest = a - high
    middle = rest.astype(bf16).astype(f32)
    return high, middle, rest - middle


def encode_rows(part, beside):
    size = jnp.abs(part)
    top = jnp.max(size, axis=1, keepdims=True)
    top = (jnp.maximum(top, 1e-30) * (1 + 2.0**-7)).astype(bf16).astype(f32)
    code = jnp.exp(size * (SPAN / top) - SPAN / 2)
    code = jnp.where(part < 0, -code, code)
    lane = lax.broadcasted_iota(jnp.int32, (24, 128), 1)
    return code.astype(bf16), jnp.where(lane == 96, top, beside).astype(bf16)


def decode_rows(code, side):
    code = code.astype(f32)
    size = (jnp.log(jnp.abs(code)) + SPAN / 2) * (side[:, 96:97] * (1 / SPAN))
    return jnp.where(code < 0, -size, size)


def placed(param):
    wide = jnp.concatenate([jnp.zeros((1, 100), f32), param, jnp.zeros((1, 4), f32)], axis=1)
    return jnp.broadcast_to(wide, (8, 128))


def pick_kernel(core_ref, tiles_ref, vector_ref, param_ref, out_ref):
    i = pl.program_id(0)

    @pl.when(i < 2)
    def _():
        out_ref[...] = tiles_ref[:, 0]

    @pl.when(i == 2)
    def _():
        out_ref[0, 0:8, :] = jnp.broadcast_to(vector_ref[...], (8, 768))
        out_ref[0, 8:16, 0:128] = placed(param_ref[...])


def pick(core, tiles, vector, param):
    return pl.pallas_call(
        pick_kernel,
        grid_spec=pltpu.PrefetchScalarGridSpec(
            num_scalar_prefetch=1,
            grid=(3,),
            in_specs=[
                pl.BlockSpec((8, 1, 24, 768), lambda i, c: (jnp.minimum(i, 1), 1 - c[0], 0, 0)),
                pl.BlockSpec((1, 768), lambda i, c: (0, 0)),
                pl.BlockSpec((1, 24), lambda i, c: (0, 0)),
            ],
            out_specs=pl.BlockSpec((8, 24, 768), lambda i, c: (i, 0, 0)),
        ),
        out_shape=pltpu.VMEM((17, 24, 768), f32),
        compiler_params=PARAMS,
        name="pick",
    )(core, tiles, vector, param)


def encode_kernel(core_ref, tiles_ref, got_ref, small_ref, vector_ref, param_ref, *refs):
    out_ref = refs[-1]
    core = core_ref[0]
    total = vector_ref[...] + small_ref[0, 0:1, :]
    wide = [jnp.concatenate([total[:, 96 * k : 96 * k + 96], jnp.zeros((1, 32), f32)], axis=1) for k in range(8)]
    mine = placed(param_ref[...])
    theirs = jnp.broadcast_to(small_ref[0, 8:9, 0:128], (8, 128))
    parts = pieces(jnp.concatenate(wide, axis=0))
    first = pieces(jnp.where(core == 0, mine, theirs))
    second = pieces(jnp.where(core == 0, theirs, mine))
    row = lax.broadcasted_iota(jnp.int32, (8, 128), 0)
    listed = jnp.zeros((8, 128), f32)
    for k, a in enumerate((*first, *second)):
        listed = jnp.where(row == k, a, listed)
    lane = lax.broadcasted_iota(jnp.int32, (8, 128), 1)
    beside = jnp.concatenate([jnp.where(lane >= 100, listed, parts[0]), parts[1], parts[2]], axis=0)
    for x in range(4):
        out_ref[x, :, 0:768], out_ref[x, :, 768:896] = encode_rows(tiles_ref[0, x, 0] + got_ref[x], beside)


def encode(core, grad, got, vector, param, message=None):
    t = int(message is not None)
    return pl.pallas_call(
        encode_kernel,
        grid_spec=pltpu.PrefetchScalarGridSpec(
            num_scalar_prefetch=1,
            grid=(4,),
            in_specs=[
                pl.BlockSpec((1, 4, 1, 24, 768), lambda i, c: (i, 0, c[0], 0, 0)),
                pl.BlockSpec((4, 24, 768), lambda i, c: (i, 0, 0)),
                pl.BlockSpec((1, 24, 768), lambda i, c: (16, 0, 0)),
                pl.BlockSpec((1, 768), lambda i, c: (0, 0)),
                pl.BlockSpec((1, 24), lambda i, c: (0, 0)),
            ] + [pl.BlockSpec(memory_space=pl.ANY)] * t,
            out_specs=pl.BlockSpec((4, 24, 896), lambda i, c: (0, 2 * i + t, 0)),
        ),
        out_shape=shape(4, 192, 896, dtype=bf16),
        input_output_aliases={6: 0} if t else {},
        compiler_params=PARAMS,
        name="encode",
    )(core, grad.reshape(4, 4, 2, 24, 768), got, got, vector, param, *([message] * t))


def recode_kernel(message_ref, out_ref):
    lane = lax.broadcasted_iota(jnp.int32, (24, 128), 1)
    to, at = (lax.broadcasted_iota(jnp.int32, (24, 24), d) for d in (0, 1))
    for t in range(2):
        vector = jnp.zeros((8, 128), f32)
        listed = jnp.zeros((24, 128), f32)
        for x in range(4):
            side = message_ref[x, 24 * t : 24 * t + 24, 768:896]
            wide = side.astype(f32)
            vector = vector + (wide[0:8] + wide[8:16] + wide[16:24])
            chosen = ((to == at + 6 * x) & (at < 6)).astype(bf16)
            listed = listed + jnp.dot(chosen, side, preferred_element_type=f32)
        beside = jnp.where(lane >= 100, listed, jnp.concatenate(pieces(vector), axis=0))
        for y in range(4):
            rows = slice(48 * y + 24 * t, 48 * y + 24 * t + 24)
            part = jnp.zeros((24, 768), f32)
            for x in range(4):
                part = part + decode_rows(message_ref[x, rows, 0:768], message_ref[x, rows, 768:896].astype(f32))
            to_y = slice(24 * t, 24 * t + 24)
            out_ref[y, to_y, 0:768], out_ref[y, to_y, 768:896] = encode_rows(part, beside)


def decode_kernel(message_ref, up_ref, down_ref, mean_ref, sizes_ref, vector_ref, params_ref):
    lane = lax.broadcasted_iota(jnp.int32, (24, 128), 1)
    for t, param_ref in enumerate((up_ref, down_ref)):
        rows = slice(24 * t, 24 * t + 24)
        total = jnp.zeros((24, 768), f32)
        beside = jnp.zeros((24, 128), f32)
        for y in range(4):
            side = message_ref[y, rows, 768:896].astype(f32)
            params_ref[t, y] = side
            beside = beside + side
            total = total + decode_rows(message_ref[y, rows, 0:768], side)
        mean = total * 32**-0.5
        mean_ref[rows] = mean
        vector_ref[t] = beside[0:8] + beside[8:16] + beside[16:24]
        param = param_ref[...]
        own = jnp.sum(param * param, axis=1, keepdims=True)
        size = jnp.sum(mean * mean, axis=1, keepdims=True)
        both = jnp.where(lane < 64, own, size)
        for m in range(4):
            sizes_ref[m, rows] = both


def step_kernel(up_ref, down_ref, mean_ref, sizes_ref, next_up_ref, next_down_ref, copies_ref):
    for t, (param_ref, next_ref) in enumerate(((up_ref, next_up_ref), (down_ref, next_down_ref))):
        rows = slice(24 * t, 24 * t + 24)
        sizes = (sizes_ref[0, rows] + sizes_ref[1, rows]) + (sizes_ref[2, rows] + sizes_ref[3, rows])
        ratio = jnp.sqrt(sizes[:, 0:1]) * lax.rsqrt(sizes[:, 64:65] + 1e-06)
        after = param_ref[...] - learn_rate * (mean_ref[rows] * ratio)
        next_ref[...] = after
        half = after.astype(bf16)
        for y in range(4):
            copies_ref[y, rows] = half


def merge_kernel(core_ref, plane_ref, got_ref, up_ref, down_ref):
    even = core_ref[0] == 0
    columns = []
    for y in range(2):
        for x in range(4):
            mine, other = plane_ref[x, y], got_ref[x, y]
            for c, pair in enumerate((jnp.where(even, mine, other), jnp.where(even, other, mine))):
                up_ref[y, x, c] = pair[0:24]
                columns.append(pair.astype(f32)[24:48])
    down_ref[...] = jnp.concatenate(columns, axis=0).T.astype(bf16)


def merge(core, plane, got):
    up, down = pl.pallas_call(
        merge_kernel,
        grid_spec=pltpu.PrefetchScalarGridSpec(
            num_scalar_prefetch=1,
            grid=(2,),
            in_specs=[pl.BlockSpec((4, 2, 48, 768), lambda i, c: (0, i, 0, 0))] * 2,
            out_specs=(
                pl.BlockSpec((2, 4, 2, 24, 768), lambda i, c: (i, 0, 0, 0, 0)),
                pl.BlockSpec((768, 384), lambda i, c: (0, i)),
            ),
        ),
        out_shape=(shape(4, 4, 2, 24, 768, dtype=bf16), shape(768, 768, dtype=bf16)),
        compiler_params=PARAMS,
        name="merge",
    )(core, plane, got)
    return up.reshape(768, 768), down


def vector_kernel(vectors_ref, params_ref, out_ref):
    for t in range(2):
        total = jnp.concatenate([vectors_ref[t, k : k + 1, 0:96] for k in range(8)], axis=1)
        listed = []
        for y in range(4):
            for k in range(0, 24, 3):
                param = params_ref[t, y, k : k + 1] + params_ref[t, y, k + 1 : k + 2] + params_ref[t, y, k + 2 : k + 3]
                listed.append(param[:, 100:124])
        out_ref[t : t + 1] = jnp.concatenate(listed, axis=1) - learn_rate * (total * 32**-0.5)


def exchange(a, axis):
    return lax.all_to_all(a, axis, 0, 0, tiled=True)


def on_device(
    slope_up, slope_down, slope_norm, slope_bias, param_up, param_down, param_norm, param_bias
):
    cores = lax.axis_index("core").astype(jnp.int32).reshape(1)
    turned = param_down.T
    message = None
    for grad, vector, param in ((slope_up[0], slope_norm, param_norm), (slope_down[0].T, slope_bias, param_bias)):
        param = param.reshape(1, 24)
        first = (grad.reshape(16, 2, 24, 768), vector, param)
        got = lax.ppermute(pick(cores, *(first if message is not None else in_hbm(*first))), "core", SWAP)
        message = encode(cores, grad, got, vector, param, message)
    recoded = call(recode_kernel, shape(4, 48, 896, dtype=bf16), 1)(exchange(message, "x"))
    outs = (shape(48, 768), shape(4, 48, 128), shape(2, 8, 128), shape(2, 4, 24, 128))
    mean, sizes, vectors, params = call(decode_kernel, outs, 3)(exchange(recoded, "y"), param_up, turned)
    outs = (shape(24, 768), shape(24, 768), shape(4, 48, 768, dtype=bf16))
    next_up, next_down, copies = call(step_kernel, outs, 4)(param_up, turned, mean, exchange(sizes, MODEL))
    rows = exchange(copies, "y")
    norm, bias = call(vector_kernel, shape(2, 768), 2)(vectors, params)
    at = 24 * lax.axis_index(("y", "x", "core"))
    plane = exchange(jnp.broadcast_to(rows[None], (4, 4, 48, 768)), "x")
    half_up, half_down = merge(cores, plane, lax.ppermute(plane, "core", SWAP))
    return (
        half_up, half_down, norm.astype(bf16), bias.astype(bf16), next_up, next_down.T,
        lax.dynamic_slice_in_dim(norm, at, 24), lax.dynamic_slice_in_dim(bias, at, 24),
    )


def solution(mesh):
    split = Mesh(
        mesh.devices.reshape(mesh.shape["ens"], 4, 4, 2, 2, 2),
        ("ens", "y", "x", "core", "mz", "my"),
    )
    return jax.shard_map(
        on_device,
        mesh=split,
        in_specs=(
            P(ENS_REPLICA, None, MODEL),
            P(ENS_REPLICA, MODEL, None),
            P(ENS_REPLICA, None),
            P(ENS_REPLICA, None),
            P(ENS_REPLICA, MODEL),
            P(("ens", *MODEL), ("y", "x", "core")),
            P(ENS_REPLICA),
            P(ENS_REPLICA),
        ),
        out_specs=(
            P("ens", MODEL),
            P(("ens", *MODEL), None),
            P("ens"),
            P("ens"),
            P(ENS_REPLICA, MODEL),
            P(("ens", *MODEL), ("y", "x", "core")),
            P(ENS_REPLICA),
            P(ENS_REPLICA),
        ),
        check_vma=False,
    )
```

```python
import jax
import jax.numpy as jnp
from jax import lax
from jax.experimental import pallas as pl
from jax.experimental.pallas import tpu as pltpu
from jax.sharding import Mesh
from jax.sharding import PartitionSpec as P

ENS_REPLICA = ("ens", "y", "x", "core")
MODEL = ("mz", "my")
SWAP = [(0, 1), (1, 0)]

learn_rate = 0.4
f32 = jnp.float32
bf16 = jnp.bfloat16
SPAN = 173.25
VMEM = pl.BlockSpec(memory_space=pltpu.VMEM)
PARAMS = pltpu.CompilerParams(vmem_limit_bytes=12 << 20)


def in_hbm(*arrays):
    return [pltpu.with_memory_space_constraint(a, pltpu.HBM) for a in arrays]


def shape(*dims, dtype=f32):
    return jax.ShapeDtypeStruct(dims, dtype)


def call(kernel, out_shape, count):
    return pl.pallas_call(
        kernel,
        in_specs=[VMEM] * count,
        out_specs=jax.tree.map(lambda _: VMEM, out_shape),
        out_shape=out_shape,
        compiler_params=PARAMS,
    )


def pieces(a):
    high = a.astype(bf16).astype(f32)
    rest = a - high
    middle = rest.astype(bf16).astype(f32)
    return high, middle, rest - middle


def encode_rows(part):
    size = jnp.abs(part)
    top = jnp.max(size, axis=1, keepdims=True)
    top = (jnp.maximum(top, 1e-30) * (1 + 2.0**-7)).astype(bf16).astype(f32)
    code = jnp.exp(size * (SPAN / top) - SPAN / 2)
    return jnp.where(part < 0, -code, code).astype(bf16), top


def decode_rows(code, top):
    code = code.astype(f32)
    size = (jnp.log(jnp.abs(code)) + SPAN / 2) * (top * (1 / SPAN))
    return jnp.where(code < 0, -size, size)


def diagonal(width, first):
    row, lane = (lax.broadcasted_iota(jnp.int32, (24, width), d) for d in (0, 1))
    return lane == row + first


def laid(top, width, first):
    return jnp.sum(jnp.where(diagonal(width, first), top, 0.0), axis=0, keepdims=True)


def stood(lanes, first):
    return jnp.sum(jnp.where(diagonal(lanes.shape[1], first), lanes, 0.0), axis=1, keepdims=True)


def padded(before, a, width):
    parts = [jnp.zeros((1, before), f32)] * (before > 0) + [a]
    after = width - before - a.shape[1]
    return jnp.concatenate(parts + [jnp.zeros((1, after), f32)] * (after > 0), axis=1)


def pick_up_kernel(core_ref, tiles_ref, vector_ref, param_ref, out_ref):
    i = pl.program_id(0)

    @pl.when(i < 2)
    def _():
        out_ref[...] = tiles_ref[:, 0]

    @pl.when(i == 2)
    def _():
        out_ref[0, 0:8, :] = jnp.broadcast_to(vector_ref[...], (8, 768))
        out_ref[0, 8:16, :] = jnp.broadcast_to(padded(0, param_ref[...], 768), (8, 768))


def pick_down_kernel(core_ref, tiles_ref, vector_ref, param_ref, out_ref, mine_ref):
    i = pl.program_id(0)

    @pl.when(i < 2)
    def _():
        rows = tiles_ref[...].T
        even = core_ref[0] == 0
        for o in range(8):
            first, second = rows[48 * o : 48 * o + 24], rows[48 * o + 24 : 48 * o + 48]
            mine_ref[o] = jnp.where(even, first, second)
            out_ref[o] = jnp.where(even, second, first)

    @pl.when(i == 2)
    def _():
        out_ref[0, 0:8, :] = jnp.broadcast_to(vector_ref[...], (8, 768))
        out_ref[0, 8:16, :] = jnp.broadcast_to(padded(0, param_ref[...], 768), (8, 768))


VECTOR_SPECS = [pl.BlockSpec((1, 768), lambda i, c: (0, 0)), pl.BlockSpec((1, 24), lambda i, c: (0, 0))]


def pick_up(core, tiles, vector, param):
    return pl.pallas_call(
        pick_up_kernel,
        grid_spec=pltpu.PrefetchScalarGridSpec(
            num_scalar_prefetch=1,
            grid=(3,),
            in_specs=[pl.BlockSpec((8, 1, 24, 768), lambda i, c: (jnp.minimum(i, 1), 1 - c[0], 0, 0)), *VECTOR_SPECS],
            out_specs=pl.BlockSpec((8, 24, 768), lambda i, c: (i, 0, 0)),
        ),
        out_shape=pltpu.VMEM((17, 24, 768), f32),
        compiler_params=PARAMS,
        name="pick_up",
    )(core, tiles, vector, param)


def pick_down(core, grad, vector, param):
    return pl.pallas_call(
        pick_down_kernel,
        grid_spec=pltpu.PrefetchScalarGridSpec(
            num_scalar_prefetch=1,
            grid=(3,),
            in_specs=[pl.BlockSpec((768, 384), lambda i, c: (0, jnp.minimum(i, 1))), *VECTOR_SPECS],
            out_specs=(
                pl.BlockSpec((8, 24, 768), lambda i, c: (i, 0, 0)),
                pl.BlockSpec((8, 24, 768), lambda i, c: (jnp.minimum(i, 1), 0, 0)),
            ),
        ),
        out_shape=(pltpu.VMEM((17, 24, 768), f32), pltpu.VMEM((16, 24, 768), f32)),
        compiler_params=PARAMS,
        name="pick_down",
    )(core, grad, vector, param)


def vector_rows(t, core, small_ref, vector_ref, param_ref):
    parts = pieces(vector_ref[...] + small_ref[0, 0:1, :])
    mine, theirs = param_ref[...], small_ref[0, 8:9, 0:24]
    pairs = (jnp.where(core == 0, mine, theirs), jnp.where(core == 0, theirs, mine))
    listed = padded(144 * t, jnp.concatenate([p for pair in pairs for p in pieces(pair)], axis=1), 768)
    row = lax.broadcasted_iota(jnp.int32, (8, 768), 0)
    rows = jnp.where(row == 7, listed, 0.0)
    for k in range(3):
        rows = jnp.where(row == 1 + 3 * t + k, parts[k], rows)
    return rows


def encode_up_kernel(core_ref, mine_ref, got_ref, small_ref, vector_ref, param_ref, out_ref, rows_ref):
    y = pl.program_id(0)

    @pl.when(y == 0)
    def _():
        rows = vector_rows(0, core_ref[0], small_ref, vector_ref, param_ref)
        for x in range(4):
            rows_ref[x] = rows

    for x in range(4):
        out_ref[x], top = encode_rows(mine_ref[0, x, 0] + got_ref[x])
        rows_ref[x, 0:1, 0:256] += laid(top, 256, 48 * y)


def encode_down_kernel(core_ref, mine_ref, got_ref, small_ref, vector_ref, param_ref, before_ref, message_ref, out_ref, rows_ref):
    y = pl.program_id(0)

    @pl.when(y == 0)
    def _():
        rows = vector_rows(1, core_ref[0], small_ref, vector_ref, param_ref)
        for x in range(4):
            rows_ref[x] = before_ref[x] + rows

    @pl.when(y < 4)
    def _():
        for x in range(4):
            out_ref[x], top = encode_rows(mine_ref[x] + got_ref[x])
            rows_ref[x, 0:1, 0:256] += laid(top, 256, 48 * y + 24)

    @pl.when(y == 4)
    def _():
        for x in range(4):
            out_ref[x, 0:8] = rows_ref[x].astype(bf16)


SMALL_SPECS = [
    pl.BlockSpec((4, 24, 768), lambda i, c: (jnp.minimum(i, 3), 0, 0)),
    pl.BlockSpec((1, 24, 768), lambda i, c: (16, 0, 0)),
    *VECTOR_SPECS,
]


def encode_up(core, grad, got, vector, param):
    return pl.pallas_call(
        encode_up_kernel,
        grid_spec=pltpu.PrefetchScalarGridSpec(
            num_scalar_prefetch=1,
            grid=(4,),
            in_specs=[pl.BlockSpec((1, 4, 1, 24, 768), lambda i, c: (i, 0, c[0], 0, 0)), *SMALL_SPECS],
            out_specs=(
                pl.BlockSpec((4, 24, 768), lambda i, c: (0, 2 * i, 0)),
                pl.BlockSpec((4, 8, 768), lambda i, c: (0, 0, 0)),
            ),
        ),
        out_shape=(shape(4, 200, 768, dtype=bf16), shape(4, 8, 768)),
        compiler_params=PARAMS,
        name="encode_up",
    )(core, grad.reshape(4, 4, 2, 24, 768), got, got, vector, param)


def encode_down(core, mine, got, vector, param, before, message):
    return pl.pallas_call(
        encode_down_kernel,
        grid_spec=pltpu.PrefetchScalarGridSpec(
            num_scalar_prefetch=1,
            grid=(5,),
            in_specs=[
                pl.BlockSpec((4, 24, 768), lambda i, c: (jnp.minimum(i, 3), 0, 0)),
                *SMALL_SPECS,
                pl.BlockSpec((4, 8, 768), lambda i, c: (0, 0, 0)),
                pl.BlockSpec(memory_space=pl.ANY),
            ],
            out_specs=pl.BlockSpec((4, 24, 768), lambda i, c: (0, jnp.minimum(2 * i + 1, 8), 0)),
            scratch_shapes=[pltpu.VMEM((4, 8, 768), f32)],
        ),
        out_shape=shape(4, 200, 768, dtype=bf16),
        input_output_aliases={7: 0},
        compiler_params=PARAMS,
        name="encode_down",
    )(core, mine, got, got, vector, param, before, message)


def recode_kernel(message_ref, out_ref):
    beside = [message_ref[x, 192:200, :].astype(f32) for x in range(4)]
    total = (beside[0] + beside[1]) + (beside[2] + beside[3])
    row = lax.broadcasted_iota(jnp.int32, (8, 768), 0)
    chips = [b[7:8, 0:288] for b in beside]
    rows = jnp.where(row == 7, padded(0, jnp.concatenate(chips[0:2], axis=1), 768), 0.0)
    rows = jnp.where(row == 0, padded(128, jnp.concatenate(chips[2:4], axis=1), 768), rows)
    for t in range(2):
        parts = pieces(total[1 + 3 * t : 2 + 3 * t] + total[2 + 3 * t : 3 + 3 * t] + total[3 + 3 * t : 4 + 3 * t])
        for k in range(3):
            rows = jnp.where(row == 1 + 3 * t + k, parts[k], rows)
    for y in range(4):
        tops = jnp.zeros((1, 128), f32)
        for t in range(2):
            at = 48 * y + 24 * t
            part = jnp.zeros((24, 768), f32)
            for x in range(4):
                part = part + decode_rows(message_ref[x, at : at + 24, :], stood(beside[x][0:1, 0:256], at))
            out_ref[y, 24 * t : 24 * t + 24, :], top = encode_rows(part)
            tops = tops + laid(top, 128, 24 * t)
        out_ref[y, 48:56, :] = (rows + jnp.where(row == 0, padded(0, tops, 768), 0.0)).astype(bf16)


def decode_kernel(message_ref, up_ref, down_ref, mean_ref, sizes_ref, vector_ref, params_ref):
    lane = lax.broadcasted_iota(jnp.int32, (24, 128), 1)
    beside = [message_ref[y, 48:56, :].astype(f32) for y in range(4)]
    total = (beside[0] + beside[1]) + (beside[2] + beside[3])
    for y in range(4):
        params_ref[y] = beside[y]
    for t, param_ref in enumerate((up_ref, down_ref)):
        rows = slice(24 * t, 24 * t + 24)
        mean = jnp.zeros((24, 768), f32)
        for y in range(4):
            mean = mean + decode_rows(message_ref[y, rows, :], stood(beside[y][0:1, 0:128], 24 * t))
        mean = mean * 32**-0.5
        mean_ref[rows] = mean
        vector_ref[t : t + 1] = total[1 + 3 * t : 2 + 3 * t] + total[2 + 3 * t : 3 + 3 * t] + total[3 + 3 * t : 4 + 3 * t]
        param = param_ref[...]
        own = jnp.sum(param * param, axis=1, keepdims=True)
        size = jnp.sum(mean * mean, axis=1, keepdims=True)
        both = jnp.where(lane < 64, own, size)
        for m in range(4):
            sizes_ref[m, rows] = both


def step_kernel(up_ref, down_ref, mean_ref, sizes_ref, next_up_ref, next_down_ref, copies_ref):
    for t, (param_ref, next_ref) in enumerate(((up_ref, next_up_ref), (down_ref, next_down_ref))):
        rows = slice(24 * t, 24 * t + 24)
        sizes = (sizes_ref[0, rows] + sizes_ref[1, rows]) + (sizes_ref[2, rows] + sizes_ref[3, rows])
        ratio = jnp.sqrt(sizes[:, 0:1]) * lax.rsqrt(sizes[:, 64:65] + 1e-06)
        after = param_ref[...] - learn_rate * (mean_ref[rows] * ratio)
        next_ref[...] = after
        half = after.astype(bf16)
        for y in range(4):
            copies_ref[y, rows] = half


def merge_kernel(core_ref, plane_ref, got_ref, up_ref, down_ref):
    even = core_ref[0] == 0
    columns = []
    for y in range(2):
        for x in range(4):
            mine, other = plane_ref[x, y], got_ref[x, y]
            for c, pair in enumerate((jnp.where(even, mine, other), jnp.where(even, other, mine))):
                up_ref[y, x, c] = pair[0:24]
                columns.append(pair.astype(f32)[24:48])
    down_ref[...] = jnp.concatenate(columns, axis=0).T.astype(bf16)


def merge(core, plane, got):
    up, down = pl.pallas_call(
        merge_kernel,
        grid_spec=pltpu.PrefetchScalarGridSpec(
            num_scalar_prefetch=1,
            grid=(2,),
            in_specs=[pl.BlockSpec((4, 2, 48, 768), lambda i, c: (0, i, 0, 0))] * 2,
            out_specs=(
                pl.BlockSpec((2, 4, 2, 24, 768), lambda i, c: (i, 0, 0, 0, 0)),
                pl.BlockSpec((768, 384), lambda i, c: (0, i)),
            ),
        ),
        out_shape=(shape(4, 4, 2, 24, 768, dtype=bf16), shape(768, 768, dtype=bf16)),
        compiler_params=PARAMS,
        name="merge",
    )(core, plane, got)
    return up.reshape(768, 768), down


def vector_kernel(vectors_ref, params_ref, out_ref):
    for t in range(2):
        listed = []
        for y in range(4):
            for x in range(4):
                row, first = (7, 288 * x) if x < 2 else (0, 128 + 288 * (x - 2))
                for c in range(2):
                    at = first + 144 * t + 72 * c
                    lanes = params_ref[y, row : row + 1, at : at + 72]
                    listed.append(lanes[:, 0:24] + lanes[:, 24:48] + lanes[:, 48:72])
        out_ref[t : t + 1] = jnp.concatenate(listed, axis=1) - learn_rate * (vectors_ref[t : t + 1] * 32**-0.5)


def exchange(a, axis):
    return lax.all_to_all(a, axis, 0, 0, tiled=True)


def on_device(
    slope_up, slope_down, slope_norm, slope_bias, param_up, param_down, param_norm, param_bias
):
    cores = lax.axis_index("core").astype(jnp.int32).reshape(1)
    turned = param_down.T
    norms = (slope_norm, param_norm.reshape(1, 24))
    biases = (slope_bias, param_bias.reshape(1, 24))
    sent_up = pick_up(cores, *in_hbm(slope_up[0].reshape(16, 2, 24, 768), *norms))
    got_up = lax.ppermute(sent_up, "core", SWAP)
    sent_down, mine_down = pick_down(cores, slope_down[0], *biases)
    got_down = lax.ppermute(sent_down, "core", SWAP)
    message, rows = encode_up(cores, slope_up[0], got_up, *norms)
    message = encode_down(cores, mine_down, got_down, *biases, rows, message)
    recoded = call(recode_kernel, shape(4, 56, 768, dtype=bf16), 1)(exchange(message, "x"))
    outs = (shape(48, 768), shape(4, 48, 128), shape(2, 768), shape(4, 8, 768))
    mean, sizes, vectors, params = call(decode_kernel, outs, 3)(exchange(recoded, "y"), param_up, turned)
    outs = (shape(24, 768), shape(24, 768), shape(4, 48, 768, dtype=bf16))
    next_up, next_down, copies = call(step_kernel, outs, 4)(param_up, turned, mean, exchange(sizes, MODEL))
    rows = exchange(copies, "y")
    norm, bias = call(vector_kernel, shape(2, 768), 2)(vectors, params)
    at = 24 * lax.axis_index(("y", "x", "core"))
    plane = exchange(jnp.broadcast_to(rows[None], (4, 4, 48, 768)), "x")
    half_up, half_down = merge(cores, plane, lax.ppermute(plane, "core", SWAP))
    return (
        half_up, half_down, norm.astype(bf16), bias.astype(bf16), next_up, next_down.T,
        lax.dynamic_slice_in_dim(norm, at, 24), lax.dynamic_slice_in_dim(bias, at, 24),
    )


def solution(mesh):
    split = Mesh(
        mesh.devices.reshape(mesh.shape["ens"], 4, 4, 2, 2, 2),
        ("ens", "y", "x", "core", "mz", "my"),
    )
    return jax.shard_map(
        on_device,
        mesh=split,
        in_specs=(
            P(ENS_REPLICA, None, MODEL),
            P(ENS_REPLICA, MODEL, None),
            P(ENS_REPLICA, None),
            P(ENS_REPLICA, None),
            P(ENS_REPLICA, MODEL),
            P(("ens", *MODEL), ("y", "x", "core")),
            P(ENS_REPLICA),
            P(ENS_REPLICA),
        ),
        out_specs=(
            P("ens", MODEL),
            P(("ens", *MODEL), None),
            P("ens"),
            P("ens"),
            P(ENS_REPLICA, MODEL),
            P(("ens", *MODEL), ("y", "x", "core")),
            P(ENS_REPLICA),
            P(ENS_REPLICA),
        ),
        check_vma=False,
    )
```

```python
import jax
import jax.numpy as jnp
from jax import lax
from jax.experimental import pallas as pl
from jax.experimental.pallas import tpu as pltpu
from jax.sharding import Mesh
from jax.sharding import PartitionSpec as P

REPLICA = ("ya", "yb", "x", "core")
ENS_REPLICA = ("ens", *REPLICA)
MODEL = ("mz", "my")
SWAP = [(0, 1), (1, 0)]

learn_rate = 0.4
f32 = jnp.float32
bf16 = jnp.bfloat16
SPAN = 173.25
VMEM = pl.BlockSpec(memory_space=pltpu.VMEM)
PARAMS = pltpu.CompilerParams(vmem_limit_bytes=12 << 20)


def in_hbm(*arrays):
    return [pltpu.with_memory_space_constraint(a, pltpu.HBM) for a in arrays]


def shape(*dims, dtype=f32):
    return jax.ShapeDtypeStruct(dims, dtype)


def call(kernel, out_shape, count):
    return pl.pallas_call(
        kernel,
        in_specs=[VMEM] * count,
        out_specs=jax.tree.map(lambda _: VMEM, out_shape),
        out_shape=out_shape,
        compiler_params=PARAMS,
    )


def pieces(a):
    high = a.astype(bf16).astype(f32)
    rest = a - high
    middle = rest.astype(bf16).astype(f32)
    return high, middle, rest - middle


def encode_rows(part):
    size = jnp.abs(part)
    top = jnp.max(size, axis=1, keepdims=True)
    top = (jnp.maximum(top, 1e-30) * (1 + 2.0**-7)).astype(bf16).astype(f32)
    code = jnp.exp(size * (SPAN / top) - SPAN / 2)
    return jnp.where(part < 0, -code, code).astype(bf16), top


def decode_rows(code, top):
    code = code.astype(f32)
    size = (jnp.log(jnp.abs(code)) + SPAN / 2) * (top * (1 / SPAN))
    return jnp.where(code < 0, -size, size)


def diagonal(width, first):
    row, lane = (lax.broadcasted_iota(jnp.int32, (24, width), d) for d in (0, 1))
    return lane == row + first


def laid(top, width, first):
    return jnp.sum(jnp.where(diagonal(width, first), top, 0.0), axis=0, keepdims=True)


def stood(lanes, first):
    return jnp.sum(jnp.where(diagonal(lanes.shape[1], first), lanes, 0.0), axis=1, keepdims=True)


def padded(before, a, width):
    parts = [jnp.zeros((1, before), f32)] * (before > 0) + [a]
    after = width - before - a.shape[1]
    return jnp.concatenate(parts + [jnp.zeros((1, after), f32)] * (after > 0), axis=1)


def pick_up_kernel(core_ref, tiles_ref, vector_ref, param_ref, out_ref):
    i = pl.program_id(0)

    @pl.when(i < 2)
    def _():
        out_ref[...] = tiles_ref[:, 0]

    @pl.when(i == 2)
    def _():
        out_ref[0, 0:8, :] = jnp.broadcast_to(vector_ref[...], (8, 768))
        out_ref[0, 8:16, :] = jnp.broadcast_to(padded(0, param_ref[...], 768), (8, 768))


def pick_down_kernel(core_ref, tiles_ref, vector_ref, param_ref, out_ref, mine_ref):
    i = pl.program_id(0)

    @pl.when(i < 2)
    def _():
        rows = tiles_ref[...].T
        even = core_ref[0] == 0
        for o in range(8):
            first, second = rows[48 * o : 48 * o + 24], rows[48 * o + 24 : 48 * o + 48]
            mine_ref[o] = jnp.where(even, first, second)
            out_ref[o] = jnp.where(even, second, first)

    @pl.when(i == 2)
    def _():
        out_ref[0, 0:8, :] = jnp.broadcast_to(vector_ref[...], (8, 768))
        out_ref[0, 8:16, :] = jnp.broadcast_to(padded(0, param_ref[...], 768), (8, 768))


VECTOR_SPECS = [pl.BlockSpec((1, 768), lambda i, c: (0, 0)), pl.BlockSpec((1, 24), lambda i, c: (0, 0))]


def pick_up(core, tiles, vector, param):
    return pl.pallas_call(
        pick_up_kernel,
        grid_spec=pltpu.PrefetchScalarGridSpec(
            num_scalar_prefetch=1,
            grid=(3,),
            in_specs=[pl.BlockSpec((8, 1, 24, 768), lambda i, c: (jnp.minimum(i, 1), 1 - c[0], 0, 0)), *VECTOR_SPECS],
            out_specs=pl.BlockSpec((8, 24, 768), lambda i, c: (i, 0, 0)),
        ),
        out_shape=pltpu.VMEM((17, 24, 768), f32),
        compiler_params=PARAMS,
        name="pick_up",
    )(core, tiles, vector, param)


def pick_down(core, grad, vector, param):
    return pl.pallas_call(
        pick_down_kernel,
        grid_spec=pltpu.PrefetchScalarGridSpec(
            num_scalar_prefetch=1,
            grid=(3,),
            in_specs=[pl.BlockSpec((768, 384), lambda i, c: (0, jnp.minimum(i, 1))), *VECTOR_SPECS],
            out_specs=(
                pl.BlockSpec((8, 24, 768), lambda i, c: (i, 0, 0)),
                pl.BlockSpec((8, 24, 768), lambda i, c: (jnp.minimum(i, 1), 0, 0)),
            ),
        ),
        out_shape=(pltpu.VMEM((17, 24, 768), f32), pltpu.VMEM((16, 24, 768), f32)),
        compiler_params=PARAMS,
        name="pick_down",
    )(core, grad, vector, param)


def vector_rows(t, core, small_ref, vector_ref, param_ref):
    parts = pieces(vector_ref[...] + small_ref[0, 0:1, :])
    mine, theirs = param_ref[...], small_ref[0, 8:9, 0:24]
    pairs = (jnp.where(core == 0, mine, theirs), jnp.where(core == 0, theirs, mine))
    listed = padded(144 * t, jnp.concatenate([p for pair in pairs for p in pieces(pair)], axis=1), 768)
    row = lax.broadcasted_iota(jnp.int32, (8, 768), 0)
    rows = jnp.where(row == 7, listed, 0.0)
    for k in range(3):
        rows = jnp.where(row == 1 + 3 * t + k, parts[k], rows)
    return rows


def encode_up_kernel(core_ref, mine_ref, got_ref, small_ref, vector_ref, param_ref, out_ref, rows_ref):
    y = pl.program_id(0)

    @pl.when(y == 0)
    def _():
        rows = vector_rows(0, core_ref[0], small_ref, vector_ref, param_ref)
        for d in range(8):
            rows_ref[d] = rows

    for x in range(4):
        out_ref[x], top = encode_rows(mine_ref[0, x, 0] + got_ref[x])
        rows_ref[4 * (y % 2) + x, 0:1, 0:128] += laid(top, 128, 48 * (y // 2))


def encode_down_kernel(core_ref, mine_ref, got_ref, small_ref, vector_ref, param_ref, before_ref, message_ref, out_ref, rows_ref):
    y = pl.program_id(0)

    @pl.when(y == 0)
    def _():
        rows = vector_rows(1, core_ref[0], small_ref, vector_ref, param_ref)
        for d in range(8):
            rows_ref[d] = before_ref[d] + rows

    @pl.when(y < 4)
    def _():
        for x in range(4):
            out_ref[x], top = encode_rows(mine_ref[x] + got_ref[x])
            rows_ref[4 * (y % 2) + x, 0:1, 0:128] += laid(top, 128, 48 * (y // 2) + 24)

    @pl.when(y >= 4)
    def _():
        for x in range(4):
            out_ref[x, 0:8] = rows_ref[4 * (y - 4) + x].astype(bf16)


SMALL_SPECS = [
    pl.BlockSpec((4, 24, 768), lambda i, c: (jnp.minimum(i, 3), 0, 0)),
    pl.BlockSpec((1, 24, 768), lambda i, c: (16, 0, 0)),
    *VECTOR_SPECS,
]


def encode_up(core, grad, got, vector, param):
    return pl.pallas_call(
        encode_up_kernel,
        grid_spec=pltpu.PrefetchScalarGridSpec(
            num_scalar_prefetch=1,
            grid=(4,),
            in_specs=[pl.BlockSpec((1, 4, 1, 24, 768), lambda i, c: (i, 0, c[0], 0, 0)), *SMALL_SPECS],
            out_specs=(
                pl.BlockSpec((4, 24, 768), lambda i, c: (i % 2, 2 * (i // 2), 0)),
                pl.BlockSpec((8, 8, 768), lambda i, c: (0, 0, 0)),
            ),
        ),
        out_shape=(shape(8, 104, 768, dtype=bf16), shape(8, 8, 768)),
        compiler_params=PARAMS,
        name="encode_up",
    )(core, grad.reshape(4, 4, 2, 24, 768), got, got, vector, param)


def encode_down(core, mine, got, vector, param, before, message):
    return pl.pallas_call(
        encode_down_kernel,
        grid_spec=pltpu.PrefetchScalarGridSpec(
            num_scalar_prefetch=1,
            grid=(6,),
            in_specs=[
                pl.BlockSpec((4, 24, 768), lambda i, c: (jnp.minimum(i, 3), 0, 0)),
                *SMALL_SPECS,
                pl.BlockSpec((8, 8, 768), lambda i, c: (0, 0, 0)),
                pl.BlockSpec(memory_space=pl.ANY),
            ],
            out_specs=pl.BlockSpec((4, 24, 768), lambda i, c: (i % 2, jnp.where(i < 4, 2 * (i // 2) + 1, 4), 0)),
            scratch_shapes=[pltpu.VMEM((8, 8, 768), f32)],
        ),
        out_shape=shape(8, 104, 768, dtype=bf16),
        input_output_aliases={7: 0},
        compiler_params=PARAMS,
        name="encode_down",
    )(core, mine, got, got, vector, param, before, message)


def recode_kernel(message_ref, kept_ref, rows_ref, out_ref):
    near = lax.axis_index("ya") == 0
    beside = [message_ref[d, 96:104, :].astype(f32) for d in range(8)]
    total = ((beside[0] + beside[1]) + (beside[2] + beside[3])) + ((beside[4] + beside[5]) + (beside[6] + beside[7]))
    row = lax.broadcasted_iota(jnp.int32, (16, 768), 0)
    rows = jnp.zeros((16, 768), f32)
    for k in range(4):
        pair = jnp.concatenate([beside[2 * k][7:8, 0:288], beside[2 * k + 1][7:8, 0:288]], axis=1)
        rows = jnp.where(row == 8 + k, padded(0, pair, 768), rows)
    for t in range(2):
        parts = pieces(total[1 + 3 * t : 2 + 3 * t] + total[2 + 3 * t : 3 + 3 * t] + total[3 + 3 * t : 4 + 3 * t])
        for k in range(3):
            rows = jnp.where(row == 1 + 3 * t + k, parts[k], rows)
    rows_ref[...] = rows
    tops = jnp.zeros((1, 128), f32)
    for t in range(2):
        sums = []
        for at in (24 * t, 48 + 24 * t):
            part = jnp.zeros((24, 768), f32)
            for d in range(8):
                part = part + decode_rows(message_ref[d, at : at + 24, :], stood(beside[d][0:1, 0:128], at))
            sums.append(part)
        kept_ref[24 * t : 24 * t + 24] = jnp.where(near, sums[0], sums[1])
        out_ref[24 * t : 24 * t + 24, :], top = encode_rows(jnp.where(near, sums[1], sums[0]))
        tops = tops + laid(top, 128, 24 * t)
    out_ref[48:64, :] = (rows + jnp.where(row == 0, padded(0, tops, 768), 0.0)).astype(bf16)


def decode_kernel(kept_ref, rows_ref, message_ref, up_ref, down_ref, mean_ref, sizes_ref, vector_ref, params_ref):
    near = lax.axis_index("ya") == 0
    lane = lax.broadcasted_iota(jnp.int32, (24, 128), 1)
    here = rows_ref[...]
    there = message_ref[48:64, :].astype(f32)
    total = here + there
    params_ref[0] = jnp.where(near, here, there)[8:16]
    params_ref[1] = jnp.where(near, there, here)[8:16]
    for t, param_ref in enumerate((up_ref, down_ref)):
        rows = slice(24 * t, 24 * t + 24)
        mean = (kept_ref[rows] + decode_rows(message_ref[rows, :], stood(there[0:1, 0:128], 24 * t))) * 32**-0.5
        mean_ref[rows] = mean
        vector_ref[t : t + 1] = total[1 + 3 * t : 2 + 3 * t] + total[2 + 3 * t : 3 + 3 * t] + total[3 + 3 * t : 4 + 3 * t]
        param = param_ref[...]
        own = jnp.sum(param * param, axis=1, keepdims=True)
        size = jnp.sum(mean * mean, axis=1, keepdims=True)
        both = jnp.where(lane < 64, own, size)
        for m in range(4):
            sizes_ref[m, rows] = both


def step_kernel(up_ref, down_ref, mean_ref, sizes_ref, next_up_ref, next_down_ref, copies_ref):
    for t, (param_ref, next_ref) in enumerate(((up_ref, next_up_ref), (down_ref, next_down_ref))):
        rows = slice(24 * t, 24 * t + 24)
        sizes = (sizes_ref[0, rows] + sizes_ref[1, rows]) + (sizes_ref[2, rows] + sizes_ref[3, rows])
        ratio = jnp.sqrt(sizes[:, 0:1]) * lax.rsqrt(sizes[:, 64:65] + 1e-06)
        after = param_ref[...] - learn_rate * (mean_ref[rows] * ratio)
        next_ref[...] = after
        half = after.astype(bf16)
        for y in range(4):
            copies_ref[y, rows] = half


def merge_kernel(core_ref, plane_ref, got_ref, up_ref, down_ref):
    even = core_ref[0] == 0
    columns = []
    for y in range(2):
        for x in range(4):
            mine, other = plane_ref[x, y], got_ref[x, y]
            for c, pair in enumerate((jnp.where(even, mine, other), jnp.where(even, other, mine))):
                up_ref[y, x, c] = pair[0:24]
                columns.append(pair.astype(f32)[24:48])
    down_ref[...] = jnp.concatenate(columns, axis=0).T.astype(bf16)


def merge(core, plane, got):
    up, down = pl.pallas_call(
        merge_kernel,
        grid_spec=pltpu.PrefetchScalarGridSpec(
            num_scalar_prefetch=1,
            grid=(2,),
            in_specs=[pl.BlockSpec((4, 2, 48, 768), lambda i, c: (0, i, 0, 0))] * 2,
            out_specs=(
                pl.BlockSpec((2, 4, 2, 24, 768), lambda i, c: (i, 0, 0, 0, 0)),
                pl.BlockSpec((768, 384), lambda i, c: (0, i)),
            ),
        ),
        out_shape=(shape(4, 4, 2, 24, 768, dtype=bf16), shape(768, 768, dtype=bf16)),
        compiler_params=PARAMS,
        name="merge",
    )(core, plane, got)
    return up.reshape(768, 768), down


def vector_kernel(vectors_ref, params_ref, out_ref):
    for t in range(2):
        listed = []
        for y in range(4):
            for x in range(4):
                row, first = 2 * (y % 2) + x // 2, 288 * (x % 2)
                for c in range(2):
                    at = first + 144 * t + 72 * c
                    lanes = params_ref[y // 2, row : row + 1, at : at + 72]
                    listed.append(lanes[:, 0:24] + lanes[:, 24:48] + lanes[:, 48:72])
        out_ref[t : t + 1] = jnp.concatenate(listed, axis=1) - learn_rate * (vectors_ref[t : t + 1] * 32**-0.5)


def exchange(a, axis):
    return lax.all_to_all(a, axis, 0, 0, tiled=True)


def on_device(
    slope_up, slope_down, slope_norm, slope_bias, param_up, param_down, param_norm, param_bias
):
    cores = lax.axis_index("core").astype(jnp.int32).reshape(1)
    turned = param_down.T
    norms = (slope_norm, param_norm.reshape(1, 24))
    biases = (slope_bias, param_bias.reshape(1, 24))
    sent_up = pick_up(cores, *in_hbm(slope_up[0].reshape(16, 2, 24, 768), *norms))
    got_up = lax.ppermute(sent_up, "core", SWAP)
    sent_down, mine_down = pick_down(cores, slope_down[0], *biases)
    got_down = lax.ppermute(sent_down, "core", SWAP)
    message, rows = encode_up(cores, slope_up[0], got_up, *norms)
    message = encode_down(cores, mine_down, got_down, *biases, rows, message)
    outs = (shape(48, 768), shape(16, 768), shape(64, 768, dtype=bf16))
    kept, rows, recoded = call(recode_kernel, outs, 1)(exchange(message, ("yb", "x")))
    across = lax.ppermute(recoded, "ya", SWAP)
    outs = (shape(48, 768), shape(4, 48, 128), shape(2, 768), shape(2, 8, 768))
    mean, sizes, vectors, params = call(decode_kernel, outs, 5)(kept, rows, across, param_up, turned)
    outs = (shape(24, 768), shape(24, 768), shape(4, 48, 768, dtype=bf16))
    next_up, next_down, copies = call(step_kernel, outs, 4)(param_up, turned, mean, exchange(sizes, MODEL))
    rows = exchange(copies, ("ya", "yb"))
    norm, bias = call(vector_kernel, shape(2, 768), 2)(vectors, params)
    at = 24 * lax.axis_index(REPLICA)
    plane = exchange(jnp.broadcast_to(rows[None], (4, 4, 48, 768)), "x")
    half_up, half_down = merge(cores, plane, lax.ppermute(plane, "core", SWAP))
    return (
        half_up, half_down, norm.astype(bf16), bias.astype(bf16), next_up, next_down.T,
        lax.dynamic_slice_in_dim(norm, at, 24), lax.dynamic_slice_in_dim(bias, at, 24),
    )


def solution(mesh):
    split = Mesh(
        mesh.devices.reshape(mesh.shape["ens"], 2, 2, 4, 2, 2, 2),
        ("ens", *REPLICA, "mz", "my"),
    )
    return jax.shard_map(
        on_device,
        mesh=split,
        in_specs=(
            P(ENS_REPLICA, None, MODEL),
            P(ENS_REPLICA, MODEL, None),
            P(ENS_REPLICA, None),
            P(ENS_REPLICA, None),
            P(ENS_REPLICA, MODEL),
            P(("ens", *MODEL), REPLICA),
            P(ENS_REPLICA),
            P(ENS_REPLICA),
        ),
        out_specs=(
            P("ens", MODEL),
            P(("ens", *MODEL), None),
            P("ens"),
            P("ens"),
            P(ENS_REPLICA, MODEL),
            P(("ens", *MODEL), REPLICA),
            P(ENS_REPLICA),
            P(ENS_REPLICA),
        ),
        check_vma=False,
    )
```

```python
import jax
import jax.numpy as jnp
from jax import lax
from jax.experimental import pallas as pl
from jax.experimental.pallas import tpu as pltpu
from jax.sharding import Mesh
from jax.sharding import PartitionSpec as P

REPLICA = ("ya", "yb", "x", "core")
ENS_REPLICA = ("ens", *REPLICA)
MODEL = ("mz", "my")
SWAP = [(0, 1), (1, 0)]

learn_rate = 0.4
f32 = jnp.float32
bf16 = jnp.bfloat16
SPAN = 173.25
VMEM = pl.BlockSpec(memory_space=pltpu.VMEM)
PARAMS = pltpu.CompilerParams(vmem_limit_bytes=12 << 20)


def in_hbm(*arrays):
    return [pltpu.with_memory_space_constraint(a, pltpu.HBM) for a in arrays]


def shape(*dims, dtype=f32):
    return jax.ShapeDtypeStruct(dims, dtype)


def call(kernel, out_shape, count):
    return pl.pallas_call(
        kernel,
        in_specs=[VMEM] * count,
        out_specs=jax.tree.map(lambda _: VMEM, out_shape),
        out_shape=out_shape,
        compiler_params=PARAMS,
    )


def pieces(a):
    high = a.astype(bf16).astype(f32)
    rest = a - high
    middle = rest.astype(bf16).astype(f32)
    return high, middle, rest - middle


def encode_rows(part):
    size = jnp.abs(part)
    top = jnp.max(size, axis=1, keepdims=True)
    top = (jnp.maximum(top, 1e-30) * (1 + 2.0**-7)).astype(bf16).astype(f32)
    code = jnp.exp(size * (SPAN / top) - SPAN / 2)
    return jnp.where(part < 0, -code, code).astype(bf16), top


def decode_rows(code, top):
    code = code.astype(f32)
    size = (jnp.log(jnp.abs(code)) + SPAN / 2) * (top * (1 / SPAN))
    return jnp.where(code < 0, -size, size)


def diagonal(width, first):
    row, lane = (lax.broadcasted_iota(jnp.int32, (24, width), d) for d in (0, 1))
    return lane == row + first


def laid(top, width, first):
    return jnp.sum(jnp.where(diagonal(width, first), top, 0.0), axis=0, keepdims=True)


def stood(lanes, first):
    return jnp.sum(jnp.where(diagonal(lanes.shape[1], first), lanes, 0.0), axis=1, keepdims=True)


def padded(before, a, width):
    parts = [jnp.zeros((1, before), f32)] * (before > 0) + [a]
    after = width - before - a.shape[1]
    return jnp.concatenate(parts + [jnp.zeros((1, after), f32)] * (after > 0), axis=1)


def pick_up_kernel(core_ref, tiles_ref, vector_ref, param_ref, out_ref):
    i = pl.program_id(0)

    @pl.when(i < 2)
    def _():
        out_ref[...] = tiles_ref[:, 0]

    @pl.when(i == 2)
    def _():
        out_ref[0, 0:8, :] = jnp.broadcast_to(vector_ref[...], (8, 768))
        out_ref[0, 8:16, :] = jnp.broadcast_to(padded(0, param_ref[...], 768), (8, 768))


def pick_down_kernel(core_ref, tiles_ref, vector_ref, param_ref, out_ref, mine_ref):
    i = pl.program_id(0)

    @pl.when(i < 2)
    def _():
        rows = tiles_ref[...].T
        even = core_ref[0] == 0
        for o in range(8):
            first, second = rows[48 * o : 48 * o + 24], rows[48 * o + 24 : 48 * o + 48]
            mine_ref[o] = jnp.where(even, first, second)
            out_ref[o] = jnp.where(even, second, first)

    @pl.when(i == 2)
    def _():
        out_ref[0, 0:8, :] = jnp.broadcast_to(vector_ref[...], (8, 768))
        out_ref[0, 8:16, :] = jnp.broadcast_to(padded(0, param_ref[...], 768), (8, 768))


VECTOR_SPECS = [pl.BlockSpec((1, 768), lambda i, c: (0, 0)), pl.BlockSpec((1, 24), lambda i, c: (0, 0))]


def pick_up(core, tiles, vector, param):
    return pl.pallas_call(
        pick_up_kernel,
        grid_spec=pltpu.PrefetchScalarGridSpec(
            num_scalar_prefetch=1,
            grid=(3,),
            in_specs=[pl.BlockSpec((8, 1, 24, 768), lambda i, c: (jnp.minimum(i, 1), 1 - c[0], 0, 0)), *VECTOR_SPECS],
            out_specs=pl.BlockSpec((8, 24, 768), lambda i, c: (i, 0, 0)),
        ),
        out_shape=pltpu.VMEM((17, 24, 768), f32),
        compiler_params=PARAMS,
        name="pick_up",
    )(core, tiles, vector, param)


def pick_down(core, grad, vector, param):
    return pl.pallas_call(
        pick_down_kernel,
        grid_spec=pltpu.PrefetchScalarGridSpec(
            num_scalar_prefetch=1,
            grid=(3,),
            in_specs=[pl.BlockSpec((768, 384), lambda i, c: (0, jnp.minimum(i, 1))), *VECTOR_SPECS],
            out_specs=(
                pl.BlockSpec((8, 24, 768), lambda i, c: (i, 0, 0)),
                pl.BlockSpec((8, 24, 768), lambda i, c: (jnp.minimum(i, 1), 0, 0)),
            ),
        ),
        out_shape=(pltpu.VMEM((17, 24, 768), f32), pltpu.VMEM((16, 24, 768), f32)),
        compiler_params=PARAMS,
        name="pick_down",
    )(core, grad, vector, param)


def vector_rows(t, core, small_ref, vector_ref, param_ref):
    parts = pieces(vector_ref[...] + small_ref[0, 0:1, :])
    mine, theirs = param_ref[...], small_ref[0, 8:9, 0:24]
    pairs = (jnp.where(core == 0, mine, theirs), jnp.where(core == 0, theirs, mine))
    listed = padded(144 * t, jnp.concatenate([p for pair in pairs for p in pieces(pair)], axis=1), 768)
    row = lax.broadcasted_iota(jnp.int32, (8, 768), 0)
    rows = jnp.where(row == 7, listed, 0.0)
    for k in range(3):
        rows = jnp.where(row == 1 + 3 * t + k, parts[k], rows)
    return rows


def encode_up_kernel(core_ref, mine_ref, got_ref, small_ref, vector_ref, param_ref, out_ref, rows_ref):
    y = pl.program_id(0)

    @pl.when(y == 0)
    def _():
        rows = vector_rows(0, core_ref[0], small_ref, vector_ref, param_ref)
        for d in range(8):
            rows_ref[d] = rows

    for x in range(4):
        out_ref[x], top = encode_rows(mine_ref[0, x, 0] + got_ref[x])
        rows_ref[4 * (y % 2) + x, 0:1, 0:128] += laid(top, 128, 48 * (y // 2))


def encode_down_kernel(core_ref, mine_ref, got_ref, small_ref, vector_ref, param_ref, before_ref, message_ref, out_ref, rows_ref):
    y = pl.program_id(0)

    @pl.when(y == 0)
    def _():
        rows = vector_rows(1, core_ref[0], small_ref, vector_ref, param_ref)
        for d in range(8):
            rows_ref[d] = before_ref[d] + rows

    @pl.when(y < 4)
    def _():
        for x in range(4):
            out_ref[x], top = encode_rows(mine_ref[x] + got_ref[x])
            rows_ref[4 * (y % 2) + x, 0:1, 0:128] += laid(top, 128, 48 * (y // 2) + 24)

    @pl.when(y >= 4)
    def _():
        for x in range(4):
            out_ref[x, 0:8] = rows_ref[4 * (y - 4) + x].astype(bf16)


SMALL_SPECS = [
    pl.BlockSpec((4, 24, 768), lambda i, c: (jnp.minimum(i, 3), 0, 0)),
    pl.BlockSpec((1, 24, 768), lambda i, c: (16, 0, 0)),
    *VECTOR_SPECS,
]


def encode_up(core, grad, got, vector, param):
    return pl.pallas_call(
        encode_up_kernel,
        grid_spec=pltpu.PrefetchScalarGridSpec(
            num_scalar_prefetch=1,
            grid=(4,),
            in_specs=[pl.BlockSpec((1, 4, 1, 24, 768), lambda i, c: (i, 0, c[0], 0, 0)), *SMALL_SPECS],
            out_specs=(
                pl.BlockSpec((4, 24, 768), lambda i, c: (i % 2, 2 * (i // 2), 0)),
                pl.BlockSpec((8, 8, 768), lambda i, c: (0, 0, 0)),
            ),
        ),
        out_shape=(shape(8, 104, 768, dtype=bf16), shape(8, 8, 768)),
        compiler_params=PARAMS,
        name="encode_up",
    )(core, grad.reshape(4, 4, 2, 24, 768), got, got, vector, param)


def encode_down(core, mine, got, vector, param, before, message):
    return pl.pallas_call(
        encode_down_kernel,
        grid_spec=pltpu.PrefetchScalarGridSpec(
            num_scalar_prefetch=1,
            grid=(6,),
            in_specs=[
                pl.BlockSpec((4, 24, 768), lambda i, c: (jnp.minimum(i, 3), 0, 0)),
                *SMALL_SPECS,
                pl.BlockSpec((8, 8, 768), lambda i, c: (0, 0, 0)),
                pl.BlockSpec(memory_space=pl.ANY),
            ],
            out_specs=pl.BlockSpec((4, 24, 768), lambda i, c: (i % 2, jnp.where(i < 4, 2 * (i // 2) + 1, 4), 0)),
            scratch_shapes=[pltpu.VMEM((8, 8, 768), f32)],
        ),
        out_shape=shape(8, 104, 768, dtype=bf16),
        input_output_aliases={7: 0},
        compiler_params=PARAMS,
        name="encode_down",
    )(core, mine, got, got, vector, param, before, message)


def recode_kernel(message_ref, kept_ref, rows_ref, out_ref):
    near = lax.axis_index("ya") == 0
    beside = [message_ref[d, 96:104, :].astype(f32) for d in range(8)]
    total = ((beside[0] + beside[1]) + (beside[2] + beside[3])) + ((beside[4] + beside[5]) + (beside[6] + beside[7]))
    row = lax.broadcasted_iota(jnp.int32, (16, 768), 0)
    rows = jnp.zeros((16, 768), f32)
    for k in range(4):
        pair = jnp.concatenate([beside[2 * k][7:8, 0:288], beside[2 * k + 1][7:8, 0:288]], axis=1)
        rows = jnp.where(row == 8 + k, padded(0, pair, 768), rows)
    for t in range(2):
        parts = pieces(total[1 + 3 * t : 2 + 3 * t] + total[2 + 3 * t : 3 + 3 * t] + total[3 + 3 * t : 4 + 3 * t])
        for k in range(3):
            rows = jnp.where(row == 1 + 3 * t + k, parts[k], rows)
    rows_ref[...] = rows
    tops = jnp.zeros((1, 128), f32)
    for t in range(2):
        sums = []
        for at in (24 * t, 48 + 24 * t):
            part = jnp.zeros((24, 768), f32)
            for d in range(8):
                part = part + decode_rows(message_ref[d, at : at + 24, :], stood(beside[d][0:1, 0:128], at))
            sums.append(part)
        kept_ref[24 * t : 24 * t + 24] = jnp.where(near, sums[0], sums[1])
        out_ref[24 * t : 24 * t + 24, :], top = encode_rows(jnp.where(near, sums[1], sums[0]))
        tops = tops + laid(top, 128, 24 * t)
    out_ref[48:64, :] = (rows + jnp.where(row == 0, padded(0, tops, 768), 0.0)).astype(bf16)


def decode_kernel(kept_ref, rows_ref, message_ref, up_ref, down_ref, mean_ref, sizes_ref, vector_ref, params_ref):
    near = lax.axis_index("ya") == 0
    lane = lax.broadcasted_iota(jnp.int32, (24, 128), 1)
    here = rows_ref[...]
    there = message_ref[48:64, :].astype(f32)
    total = here + there
    params_ref[0] = jnp.where(near, here, there)[8:16]
    params_ref[1] = jnp.where(near, there, here)[8:16]
    for t, param_ref in enumerate((up_ref, down_ref)):
        rows = slice(24 * t, 24 * t + 24)
        mean = (kept_ref[rows] + decode_rows(message_ref[rows, :], stood(there[0:1, 0:128], 24 * t))) * 32**-0.5
        mean_ref[rows] = mean
        vector_ref[t : t + 1] = total[1 + 3 * t : 2 + 3 * t] + total[2 + 3 * t : 3 + 3 * t] + total[3 + 3 * t : 4 + 3 * t]
        param = param_ref[...]
        own = jnp.sum(param * param, axis=1, keepdims=True)
        size = jnp.sum(mean * mean, axis=1, keepdims=True)
        both = jnp.where(lane < 64, own, size)
        for m in range(4):
            sizes_ref[m, rows] = both


def step_kernel(up_ref, down_ref, mean_ref, sizes_ref, next_up_ref, next_down_ref, half_ref):
    for t, (param_ref, next_ref) in enumerate(((up_ref, next_up_ref), (down_ref, next_down_ref))):
        rows = slice(24 * t, 24 * t + 24)
        sizes = (sizes_ref[0, rows] + sizes_ref[1, rows]) + (sizes_ref[2, rows] + sizes_ref[3, rows])
        ratio = jnp.sqrt(sizes[:, 0:1]) * lax.rsqrt(sizes[:, 64:65] + 1e-06)
        after = param_ref[...] - learn_rate * (mean_ref[rows] * ratio)
        next_ref[...] = after
        half_ref[rows] = after.astype(bf16)


def copies_kernel(own_ref, other_ref, out_ref):
    near = lax.axis_index("ya") == 0
    own, other = own_ref[...], other_ref[...]
    first, second = jnp.where(near, own, other), jnp.where(near, other, own)
    for d in range(8):
        out_ref[d, 0] = first
        out_ref[d, 1] = second


def merge_kernel(core_ref, plane_ref, got_ref, up_ref, down_ref):
    even = core_ref[0] == 0
    columns = []
    for y in range(2):
        for x in range(4):
            mine, other = plane_ref[4 * y + x, 0], got_ref[4 * y + x, 0]
            for c, pair in enumerate((jnp.where(even, mine, other), jnp.where(even, other, mine))):
                up_ref[y, x, c] = pair[0:24]
                columns.append(pair.astype(f32)[24:48])
    down_ref[...] = jnp.concatenate(columns, axis=0).T.astype(bf16)


def merge(core, plane, got):
    up, down = pl.pallas_call(
        merge_kernel,
        grid_spec=pltpu.PrefetchScalarGridSpec(
            num_scalar_prefetch=1,
            grid=(2,),
            in_specs=[pl.BlockSpec((8, 1, 48, 768), lambda i, c: (0, i, 0, 0))] * 2,
            out_specs=(
                pl.BlockSpec((2, 4, 2, 24, 768), lambda i, c: (i, 0, 0, 0, 0)),
                pl.BlockSpec((768, 384), lambda i, c: (0, i)),
            ),
        ),
        out_shape=(shape(4, 4, 2, 24, 768, dtype=bf16), shape(768, 768, dtype=bf16)),
        compiler_params=PARAMS,
        name="merge",
    )(core, plane, got)
    return up.reshape(768, 768), down


def vector_kernel(vectors_ref, params_ref, out_ref):
    for t in range(2):
        listed = []
        for y in range(4):
            for x in range(4):
                row, first = 2 * (y % 2) + x // 2, 288 * (x % 2)
                for c in range(2):
                    at = first + 144 * t + 72 * c
                    lanes = params_ref[y // 2, row : row + 1, at : at + 72]
                    listed.append(lanes[:, 0:24] + lanes[:, 24:48] + lanes[:, 48:72])
        out_ref[t : t + 1] = jnp.concatenate(listed, axis=1) - learn_rate * (vectors_ref[t : t + 1] * 32**-0.5)


def exchange(a, axis):
    return lax.all_to_all(a, axis, 0, 0, tiled=True)


def on_device(
    slope_up, slope_down, slope_norm, slope_bias, param_up, param_down, param_norm, param_bias
):
    cores = lax.axis_index("core").astype(jnp.int32).reshape(1)
    turned = param_down.T
    norms = (slope_norm, param_norm.reshape(1, 24))
    biases = (slope_bias, param_bias.reshape(1, 24))
    sent_up = pick_up(cores, *in_hbm(slope_up[0].reshape(16, 2, 24, 768), *norms))
    got_up = lax.ppermute(sent_up, "core", SWAP)
    sent_down, mine_down = pick_down(cores, slope_down[0], *biases)
    got_down = lax.ppermute(sent_down, "core", SWAP)
    message, rows = encode_up(cores, slope_up[0], got_up, *norms)
    message = encode_down(cores, mine_down, got_down, *biases, rows, message)
    outs = (shape(48, 768), shape(16, 768), shape(64, 768, dtype=bf16))
    kept, rows, recoded = call(recode_kernel, outs, 1)(exchange(message, ("yb", "x")))
    across = lax.ppermute(recoded, "ya", SWAP)
    outs = (shape(48, 768), shape(4, 48, 128), shape(2, 768), shape(2, 8, 768))
    mean, sizes, vectors, params = call(decode_kernel, outs, 5)(kept, rows, across, param_up, turned)
    outs = (shape(24, 768), shape(24, 768), shape(48, 768, dtype=bf16))
    next_up, next_down, half = call(step_kernel, outs, 4)(param_up, turned, mean, exchange(sizes, MODEL))
    copies = call(copies_kernel, shape(8, 2, 48, 768, dtype=bf16), 2)(half, lax.ppermute(half, "ya", SWAP))
    norm, bias = call(vector_kernel, shape(2, 768), 2)(vectors, params)
    at = 24 * lax.axis_index(REPLICA)
    plane = exchange(copies, ("yb", "x"))
    half_up, half_down = merge(cores, plane, lax.ppermute(plane, "core", SWAP))
    return (
        half_up, half_down, norm.astype(bf16), bias.astype(bf16), next_up, next_down.T,
        lax.dynamic_slice_in_dim(norm, at, 24), lax.dynamic_slice_in_dim(bias, at, 24),
    )


def solution(mesh):
    split = Mesh(
        mesh.devices.reshape(mesh.shape["ens"], 2, 2, 4, 2, 2, 2),
        ("ens", *REPLICA, "mz", "my"),
    )
    return jax.shard_map(
        on_device,
        mesh=split,
        in_specs=(
            P(ENS_REPLICA, None, MODEL),
            P(ENS_REPLICA, MODEL, None),
            P(ENS_REPLICA, None),
            P(ENS_REPLICA, None),
            P(ENS_REPLICA, MODEL),
            P(("ens", *MODEL), REPLICA),
            P(ENS_REPLICA),
            P(ENS_REPLICA),
        ),
        out_specs=(
            P("ens", MODEL),
            P(("ens", *MODEL), None),
            P("ens"),
            P("ens"),
            P(ENS_REPLICA, MODEL),
            P(("ens", *MODEL), REPLICA),
            P(ENS_REPLICA),
            P(ENS_REPLICA),
        ),
        check_vma=False,
    )
```
